1024 devices in a mesh: dp: 16 (over y, core), seq: 8 (over x), expert: 8 (over z).
Axes of the slice: x: 8, y: 8, z: 8, core: 2. Of those that a mesh axis runs over, the one named last changes fastest.
Arguments:
- queries: bfloat16 [8192, 4096], P(('dp', 'seq'), 'expert'), parts along dimension 0, may hold values from -256 to 256, as said below
- keys: bfloat16 [32768, 1024], P(('dp', 'seq'), 'expert'), parts along dimension 0, may hold values from -6 to 6
- values: bfloat16 [32768, 1024], P(('dp', 'seq'), 'expert'), parts along dimension 0, may hold values from -6 to 6
- lengths: int32 [128], P('dp'), parts along dimension 0, may hold values from 1 to 1024, 2048 in all
- routes: int32 [8192, 2], P(('dp', 'seq', 'expert')), parts along dimension 0, may hold values from 0 to 7, all different within a row; in each aligned block of 8 rows (0 to 7, 8 to 15, ...) at most 3 rows name the same one
- gates: float32 [8192, 2], P(('dp', 'seq', 'expert')), parts along dimension 0, may hold values from 0.2 to 1
- w_up: bfloat16 [8, 4096, 7168], P('expert', None, 'seq'), may hold values from -0.09375 to 0.09375
Outputs:
- expert_mix: bfloat16 [8192, 7168], P(('dp', 'seq', 'expert')), parts along dimension 0
The draws below stay inside these ranges and needn't reach their ends.
There are 16 independent parts, one for each index of `dp`. The reference program is written for one: setup_inputs(seed, part) draws one part's arguments, and reference() takes and returns one part's arrays. A program takes and returns all parts, laid end to end along the dimension named above; an argument that names none is the same for every part. Nothing has to cross between parts.
Inputs may be any that keep to these rules, and one draw needn't show every extreme that they name: `queries`: A query row's values are those of a normal draw or, in some rows, a multiple of a sum of key rows. The 8 lengths sum to 2048. `routes`: A row's two experts differ; among the 8 rows of one device no expert is named more than 3 times.
All inputs are finite; a program needn't handle non-finite values.
Results may differ from the reference program's by a relative error of at most 0.012.
Values may be sent and summed in bfloat16 or wider, within the bound.
No kernel may reach another device: no remote copies, remote signals or barrier semaphores. Data moves between devices by JAX's collectives and lax.ppermute only.
A program may use at most 32 MiB of HBM per device.

```python
import math
import jax
import jax.numpy as jnp
import numpy as np
from jax import lax

D = 4096
H = 32
KVH = 8
HD = 128
EXPERTS = 8
FFW = 7168
SHARD = 256
Q_DEV = 64
NDOC = 8
LEN = 2048
QTOK = 512
T_DEV = 8
CAP = 3


def base_keys(key):
    return jnp.clip(jax.random.normal(jax.random.fold_in(key, 71), (LEN, KVH * HD), jnp.float32), -6.0, 6.0)


def draw_keys(key, part):
    return base_keys(key).astype(jnp.bfloat16)


def draw_queries(key, part):
    drawn = jnp.clip(jax.random.normal(jax.random.fold_in(key, 72), (QTOK, H * HD), jnp.float32), -6.0, 6.0)
    return drawn.astype(jnp.bfloat16)


def block_levels(rng, dims, cuts, low, high):
    def one(axis_at, parts):
        heights = jax.random.uniform(jax.random.fold_in(jax.random.fold_in(rng, 6), axis_at), (parts,), jnp.float32, low / len(cuts), high / len(cuts))
        return jnp.repeat(jnp.exp(heights), dims[axis_at] // parts).reshape((-1,) + (1,) * (len(dims) - axis_at - 1))

    level = one(*cuts[0])
    for cut in cuts[1:]:
        level = level * one(*cut)
    return level


def profile(number_of, total, bound, lean):
    loads = [(1 << 20) // math.isqrt(rank ** lean) + 1 for rank in range(2, number_of + 1)]
    surplus, counts = total - bound - (number_of - 1), [1] * (number_of - 1)
    while surplus > 0:
        free = [i for i in range(number_of - 1) if counts[i] < bound]
        pool, budget = sum([loads[i] for i in free]), surplus
        for i in free:
            extra = min(bound - counts[i], max(1, budget * loads[i] // pool), surplus)
            counts[i] = counts[i] + extra
            surplus = surplus - extra
    return np.array([bound] + counts)


def ragged_sizes(own_key, number_of, total, limit, lean):
    if number_of == 2:
        one = jax.random.randint(own_key, (), max(1, total - limit), min(limit, total - 1) + 1)
        return jnp.stack([one, total - one])
    sizes = jnp.asarray(profile(number_of, total, limit, lean), jnp.int32)
    pairs = (number_of - 1) // 2
    giver, receiver = sizes[1:1 + 2 * pairs:2], sizes[2:2 + 2 * pairs:2]
    room = jnp.minimum(giver - 1, limit - receiver)
    moved = jax.random.randint(jax.random.fold_in(own_key, 1), (pairs,), 0, 1 << 20) % (room + 1)
    sizes = sizes.at[1:1 + 2 * pairs:2].set(giver - moved).at[2:2 + 2 * pairs:2].set(receiver + moved)
    return sizes[jax.random.permutation(jax.random.fold_in(own_key, 2), number_of)]


def deal_out(own_key, own, number, rows, number_of, top, bound, skew):
    sequence = jax.random.permutation(own_key, number_of)
    crowded, common = shares(number_of, rows * top, bound, skew, True), shares(number_of, rows * top, bound, skew, False)
    places = jnp.arange(number_of)

    def named(tallies, turn):
        used = int((tallies > 0).sum())
        fixed = max(1, used // 4)
        passed = fixed + (places - fixed + turn * (used - fixed)) % max(1, number_of - fixed)
        return jnp.zeros((number_of,), jnp.int32).at[sequence[jnp.where(places < fixed, places, passed)]].set(jnp.asarray(tallies, jnp.int32))

    tallies = jnp.where(number % 4 == 0, named(crowded, number // 4), named(common, number - number // 4 - 1))
    mixed = jax.random.permutation(jax.random.fold_in(own, 3), number_of)
    donor, receiver = mixed[0:number_of // 2 * 2:2], mixed[1:number_of // 2 * 2:2]
    room = jnp.minimum(tallies[donor] - 1, bound - tallies[receiver]) // 2
    room = jnp.where((donor == sequence[0]) | (receiver == sequence[0]) | (tallies[receiver] == 0), 0, jnp.maximum(room, 0))
    passed = jax.random.randint(jax.random.fold_in(own, 4), (number_of // 2,), 0, 1 << 20) % (room + 1)
    tallies = tallies.at[donor].add(-passed).at[receiver].add(passed)
    members = jnp.searchsorted(jnp.cumsum(tallies), jnp.arange(rows * top), side="right").astype(jnp.int32)
    listing = members.reshape(top, rows).T
    listing = listing[jax.random.permutation(jax.random.fold_in(own, 1), rows)]
    turn = jax.random.randint(jax.random.fold_in(own, 2), (rows, 1), 0, top)
    return jnp.take_along_axis(listing, (jnp.arange(top)[None, :] + turn) % top, axis=1)


def shares(amount, total, limit, skew, full):
    weights = [(1 << 20) // math.isqrt(standing ** skew) + 1 for standing in range(1, amount + 1)]
    largest = limit if full else min(limit, max(-(-total // amount), total * weights[0] // sum(weights)))
    least = 1 if total - largest >= amount - 1 else 0
    given, rest = [largest] + [least] * (amount - 1), total - largest - least * (amount - 1)
    while rest > 0:
        free = [i for i in range(1, amount) if given[i] < largest] or [i for i in range(1, amount) if given[i] < limit]
        whole, left = sum([weights[i] for i in free]), rest
        for i in free:
            extra = min(limit - given[i], max(1, left * weights[i] // whole), rest)
            given[i] = given[i] + extra
            rest = rest - extra
    return np.array(given)


def normal_values(key, shape, scale, bound, pieces=(), held_as=jnp.bfloat16):
    array = jax.random.normal(key, shape, jnp.float32) * scale
    if len(pieces) > 0:
        array = block_levels(key, shape, pieces, -0.22, 0.18) * array
    return jnp.clip(array, min=-bound, max=bound).astype(held_as)


def setup_inputs(seed: int = 0, part: int = 0) -> dict:
    key_of = jax.random.split(jax.random.key(seed), 8)
    part_splits = jax.random.split(jax.random.fold_in(key_of[7], part), 8)
    queries = draw_queries(jax.random.fold_in(jax.random.fold_in(key_of[7], part), 71), part)
    keys = draw_keys(jax.random.fold_in(jax.random.fold_in(key_of[7], part), 71), part)
    values = normal_values(part_splits[2], (LEN, KVH * HD), 1.0, 6.0, ((0, 8), (1, 8)))
    lengths = ragged_sizes(part_splits[3], NDOC, LEN, LEN // 2, 2).astype(jnp.int32)
    routes_keys = jax.random.split(jax.random.fold_in(part_splits[4], 1), QTOK // T_DEV)
    routes_turns = jax.random.permutation(jax.random.fold_in(part_splits[4], 3), QTOK // T_DEV)
    routes = jax.vmap(lambda own, number: deal_out(jax.random.fold_in(part_splits[4], 2), own, number, T_DEV, EXPERTS, 2, CAP, 2))(routes_keys, routes_turns).reshape((QTOK, 2))
    gates = jnp.clip(0.2 + 0.8 * jax.random.uniform(part_splits[5], (QTOK, 2), jnp.float32) ** block_levels(part_splits[5], (QTOK, 2), ((0, 64),), -0.2, 0.2), 0.2, 1.0)
    w_up = normal_values(key_of[6], (EXPERTS, D, FFW), D ** -0.5, 0.09375, ((0, 8), (2, 8)))
    return {"queries": queries, "keys": keys, "values": values, "lengths": lengths, "routes": routes, "gates": gates, "w_up": w_up}


def doc_index(positions, starts):
    return lax.optimization_barrier(jnp.sum((positions[:, None] >= starts[None, :]).astype(jnp.int32), axis=1)) - 1

def reference(queries, keys, values, lengths, routes, gates, w_up):
    qtok = queries.shape[0]
    rows = jnp.arange(qtok, dtype=jnp.int32)
    qpos = rows // Q_DEV * SHARD + SHARD - Q_DEV + rows % Q_DEV
    starts = (jnp.cumsum(lengths) - lengths).astype(jnp.int32)
    kpos = jnp.arange(LEN, dtype=jnp.int32)
    qdoc = doc_index(qpos, starts)
    kdoc = doc_index(kpos, starts)
    allowed = (kpos[None, :] <= qpos[:, None]) & (kdoc[None, :] == qdoc[:, None])
    group = H // KVH
    scale = 1.0 / HD ** 0.5
    q_heads = queries.astype(jnp.float32).reshape(qtok, KVH, group, HD).transpose(1, 2, 0, 3)
    k_heads = keys.astype(jnp.float32).reshape(LEN, KVH, HD).transpose(1, 0, 2)
    v_heads = values.astype(jnp.float32).reshape(LEN, KVH, HD).transpose(1, 0, 2)

    def one_head(operands):
        q_part, k_part, v_part = operands
        score = jnp.einsum('gqd,pd->gqp', q_part, k_part) * scale
        masked = jnp.where(allowed[None], score, jnp.float32(-1e+30))
        peak = lax.optimization_barrier(jnp.max(masked, axis=-1, keepdims=True))
        weight = jnp.where(allowed[None], jnp.exp(score - peak), jnp.float32(0.0))
        total = lax.optimization_barrier(jnp.sum(weight, axis=-1))
        weight_b = lax.optimization_barrier(weight.astype(jnp.bfloat16)).astype(jnp.float32)
        attended = jnp.einsum('gqp,pd->gqd', weight_b, v_part) / total[..., None]
        return attended.astype(jnp.bfloat16)
    heads_out = lax.map(one_head, (q_heads, k_heads, v_heads))
    attended = heads_out.transpose(2, 0, 1, 3).reshape(qtok, H * HD)
    feats = attended.astype(jnp.float32)
    normed = (feats * lax.rsqrt(lax.optimization_barrier(jnp.mean(feats * feats, axis=-1, keepdims=True)) + 1e-05)).astype(jnp.bfloat16)

    def per_expert(acc, operands):
        weight_e, which = operands
        upper = jnp.dot(normed, weight_e, preferred_element_type=jnp.float32)
        act = lax.optimization_barrier(jax.nn.silu(upper).astype(jnp.bfloat16)).astype(jnp.float32)
        share = lax.optimization_barrier(jnp.sum(jnp.where(routes == which, gates, jnp.float32(0.0)), axis=1))
        return (acc + share[:, None] * act, None)
    start_acc = jnp.zeros((qtok, FFW), jnp.float32)
    mixed, _ = lax.scan(per_expert, start_acc, (w_up, jnp.arange(EXPERTS, dtype=jnp.int32)))
    return mixed.astype(jnp.bfloat16)
```

```python
import jax
import jax.numpy as jnp
from jax import lax
from jax.sharding import PartitionSpec as P

HD = 128


def exchange(x, axis):
    return lax.all_to_all(x, axis, split_axis=0, concat_axis=0, tiled=True)


def to_everyone(x, axis):
    return exchange(jnp.broadcast_to(x, (lax.axis_size(axis), *x.shape)), axis)


def doc_index(positions, starts):
    return jnp.sum((positions[:, None] >= starts[None, :]).astype(jnp.int32), axis=1) - 1


def slots(routes, experts_all):
    blocks = routes.shape[0]
    flat = routes.reshape(blocks, -1)
    onehot = (flat[:, :, None] == jnp.arange(experts_all, dtype=jnp.int32)).astype(jnp.int32)
    count = flat.shape[1]
    earlier = jnp.arange(count)[:, None] > jnp.arange(count)[None, :]
    same = flat[:, :, None] == flat[:, None, :]
    return jnp.sum((same & earlier[None]).astype(jnp.int32), axis=2).reshape(routes.shape)


def shards(queries, keys, values, lengths, routes, gates, w_up):
    q_rows, width = queries.shape
    shard_len = keys.shape[0]
    kv_local = keys.shape[1] // HD
    group = width // HD // kv_local
    scale = 1.0 / HD**0.5
    seq_count = lax.axis_size("seq")
    expert_count = lax.axis_size("expert")
    experts_all = expert_count * w_up.shape[0]
    capacity = max(2, 3 * q_rows // (expert_count * expert_count))
    tok_count = routes.shape[0]
    starts = jnp.cumsum(lengths) - lengths
    qpos = (
        lax.axis_index("seq") * shard_len + shard_len - q_rows + jnp.arange(q_rows, dtype=jnp.int32)
    )
    qdoc = doc_index(qpos, starts)
    kv = to_everyone(jnp.concatenate([keys, values], axis=1), "seq")
    count = seq_count * shard_len
    kv = kv.reshape(count, 2 * kv_local * HD)
    k_all, v_all = kv[:, : kv_local * HD], kv[:, kv_local * HD :]
    row_routes = to_everyone(routes.reshape(1, -1), "expert").reshape(expert_count, tok_count, 2)

    q_split = queries.reshape(q_rows, kv_local, group, HD)
    kpos = jnp.arange(count, dtype=jnp.int32)
    allowed = (kpos[None, :] <= qpos[:, None]) & (doc_index(kpos, starts)[None, :] == qdoc[:, None])
    score = (
        jnp.einsum(
            "qkgd,pkd->kgqp",
            q_split,
            k_all.reshape(count, kv_local, HD),
            preferred_element_type=jnp.float32,
        )
        * scale
    )
    masked = jnp.where(allowed, score, jnp.float32(-1e30))
    peak = jnp.max(masked, axis=-1)
    weight = jnp.where(allowed, jnp.exp(score - peak[..., None]), jnp.float32(0.0))
    total = jnp.sum(weight, axis=-1)
    acc = jnp.einsum(
        "kgqp,pkd->kgqd",
        weight.astype(jnp.bfloat16),
        v_all.reshape(count, kv_local, HD),
        preferred_element_type=jnp.float32,
    )
    attended = (
        (acc / total[..., None]).astype(jnp.bfloat16).transpose(2, 0, 1, 3).reshape(q_rows, width)
    )

    place = slots(row_routes, experts_all)
    block = jnp.arange(expert_count, dtype=jnp.int32)[:, None, None]
    target = (row_routes * expert_count + block) * capacity + place
    total_slots = experts_all * expert_count * capacity
    target = target.reshape(q_rows, 2)
    slot_ids = jnp.arange(total_slots, dtype=jnp.int32)[:, None]
    selector = ((slot_ids == target[None, :, 0]) | (slot_ids == target[None, :, 1])).astype(
        jnp.bfloat16
    )
    outgoing = jnp.dot(selector, attended, preferred_element_type=jnp.float32).astype(jnp.bfloat16)
    per_expert = expert_count * capacity
    outgoing = outgoing.reshape(1, expert_count, per_expert, width)
    outgoing = jnp.broadcast_to(outgoing, (seq_count, expert_count, per_expert, width))
    landed = exchange(
        outgoing.reshape(seq_count * expert_count, per_expert, width), ("seq", "expert")
    )
    landed = landed.reshape(seq_count, expert_count, per_expert, width)
    feats = landed.astype(jnp.float32)
    square = jnp.sum(feats * feats, axis=(1, 3)) / (expert_count * width)
    norm = lax.rsqrt(square + 1e-05).reshape(seq_count * per_expert, 1)
    incoming = landed.transpose(0, 2, 1, 3).reshape(seq_count * per_expert, expert_count * width)
    upper = jnp.dot(incoming, w_up[0], preferred_element_type=jnp.float32) * norm
    act = jax.nn.silu(upper).astype(jnp.bfloat16)
    ff_local = act.shape[1]
    back = exchange(act.reshape(seq_count * expert_count, capacity, ff_local), ("seq", "expert"))
    back = back.reshape(seq_count, experts_all * capacity, ff_local)
    returned = back.transpose(1, 0, 2).reshape(experts_all * capacity, seq_count * ff_local)
    own = slots(routes[None], experts_all)[0]
    own_target = (routes * capacity + own).reshape(-1)
    own_selector = (
        own_target[:, None] == jnp.arange(experts_all * capacity, dtype=jnp.int32)[None, :]
    ).astype(jnp.bfloat16)
    picked = jnp.dot(own_selector, returned, preferred_element_type=jnp.float32)
    mixed = jnp.sum(picked.reshape(tok_count, 2, -1) * gates[:, :, None], axis=1)
    return mixed.astype(jnp.bfloat16)


def solution(mesh):
    placed = (
        P(("dp", "seq"), "expert"),
        P(("dp", "seq"), "expert"),
        P(("dp", "seq"), "expert"),
        P("dp"),
        P(("dp", "seq", "expert"), None),
        P(("dp", "seq", "expert"), None),
        P("expert", None, "seq"),
    )
    return jax.shard_map(
        shards,
        mesh=mesh,
        in_specs=placed,
        out_specs=P(("dp", "seq", "expert"), None),
        check_vma=False,
    )
```

```python
import jax
import jax.numpy as jnp
from jax import lax
from jax.sharding import PartitionSpec as P

HD = 128


def exchange(x, axis):
    return lax.all_to_all(x, axis, split_axis=0, concat_axis=0, tiled=True)


def to_everyone(x, axis):
    return exchange(jnp.broadcast_to(x, (lax.axis_size(axis), *x.shape)), axis)


def slots(routes, experts_all):
    blocks = routes.shape[0]
    flat = routes.reshape(blocks, -1)
    onehot = (flat[:, :, None] == jnp.arange(experts_all, dtype=jnp.int32)).astype(jnp.int32)
    count = flat.shape[1]
    earlier = jnp.arange(count)[:, None] > jnp.arange(count)[None, :]
    same = flat[:, :, None] == flat[:, None, :]
    return jnp.sum((same & earlier[None]).astype(jnp.int32), axis=2).reshape(routes.shape)


def shards(queries, keys, values, lengths, routes, gates, w_up):
    q_rows, width = queries.shape
    shard_len = keys.shape[0]
    kv_local = keys.shape[1] // HD
    group = width // HD // kv_local
    scale = 1.0 / HD**0.5
    seq_count = lax.axis_size("seq")
    expert_count = lax.axis_size("expert")
    experts_all = expert_count * w_up.shape[0]
    capacity = max(2, 3 * q_rows // (expert_count * expert_count))
    tok_count = routes.shape[0]
    starts = jnp.cumsum(lengths) - lengths
    qpos = (
        lax.axis_index("seq") * shard_len + shard_len - q_rows + jnp.arange(q_rows, dtype=jnp.int32)
    )
    reach = -(-(1024 - 1) // shard_len)
    row_routes = to_everyone(routes.reshape(1, -1), "expert").reshape(expert_count, tok_count, 2)
    kv_own = jnp.concatenate([keys, values], axis=0).reshape(2, shard_len, kv_local * HD)
    ring = [[(i, (i + d) % seq_count) for i in range(seq_count)] for d in range(reach + 1)]
    parts = [kv_own]
    for d in range(1, reach):
        parts.append(lax.ppermute(kv_own, "seq", ring[d]))
    parts.append(lax.ppermute(kv_own[:, shard_len - q_rows :], "seq", ring[reach]))
    kv = jnp.concatenate(parts[::-1], axis=1)
    k_all, v_all = kv[0], kv[1]
    count = k_all.shape[0]

    q_split = queries.reshape(q_rows, kv_local, group, HD)
    first = (lax.axis_index("seq") + 1) * shard_len - count
    kpos = first + jnp.arange(count, dtype=jnp.int32)
    begin = jnp.max(jnp.where(starts[None, :] <= qpos[:, None], starts[None, :], 0), axis=1)
    allowed = (kpos[None, :] <= qpos[:, None]) & (kpos[None, :] >= begin[:, None])
    score = (
        jnp.einsum(
            "qkgd,pkd->kgqp",
            q_split,
            k_all.reshape(count, kv_local, HD),
            preferred_element_type=jnp.float32,
        )
        * scale
    )
    masked = jnp.where(allowed, score, jnp.float32(-1e30))
    peak = jnp.max(masked, axis=-1)
    weight = jnp.where(allowed, jnp.exp(score - peak[..., None]), jnp.float32(0.0))
    total = jnp.sum(weight, axis=-1)
    acc = jnp.einsum(
        "kgqp,pkd->kgqd",
        weight.astype(jnp.bfloat16),
        v_all.reshape(count, kv_local, HD),
        preferred_element_type=jnp.float32,
    )
    attended = (
        (acc / total[..., None]).astype(jnp.bfloat16).transpose(2, 0, 1, 3).reshape(q_rows, width)
    )

    place = slots(row_routes, experts_all)
    block = jnp.arange(expert_count, dtype=jnp.int32)[:, None, None]
    target = (row_routes * expert_count + block) * capacity + place
    total_slots = experts_all * expert_count * capacity
    target = target.reshape(q_rows, 2)
    slot_ids = jnp.arange(total_slots, dtype=jnp.int32)[:, None]
    selector = ((slot_ids == target[None, :, 0]) | (slot_ids == target[None, :, 1])).astype(
        jnp.bfloat16
    )
    outgoing = jnp.dot(selector, attended, preferred_element_type=jnp.float32).astype(jnp.bfloat16)
    per_expert = expert_count * capacity
    outgoing = outgoing.reshape(1, expert_count, per_expert, width)
    outgoing = jnp.broadcast_to(outgoing, (seq_count, expert_count, per_expert, width))
    landed = exchange(
        outgoing.reshape(seq_count * expert_count, per_expert, width), ("seq", "expert")
    )
    landed = landed.reshape(seq_count, expert_count, per_expert, width)
    feats = landed.astype(jnp.float32)
    square = jnp.sum(feats * feats, axis=(1, 3)) / (expert_count * width)
    norm = lax.rsqrt(square + 1e-05).reshape(seq_count * per_expert, 1)
    incoming = landed.transpose(0, 2, 1, 3).reshape(seq_count * per_expert, expert_count * width)
    upper = jnp.dot(incoming, w_up[0], preferred_element_type=jnp.float32) * norm
    act = jax.nn.silu(upper).astype(jnp.bfloat16)
    ff_local = act.shape[1]
    back = exchange(act.reshape(seq_count * expert_count, capacity, ff_local), ("seq", "expert"))
    back = back.reshape(seq_count, experts_all * capacity, ff_local)
    returned = back.transpose(1, 0, 2).reshape(experts_all * capacity, seq_count * ff_local)
    back, routes = lax.optimization_barrier((back, routes))
    own = slots(routes[None], experts_all)[0]
    own_target = (routes * capacity + own).reshape(-1)
    own_selector = (
        own_target[:, None] == jnp.arange(experts_all * capacity, dtype=jnp.int32)[None, :]
    ).astype(jnp.bfloat16)
    picked = jnp.dot(own_selector, returned, preferred_element_type=jnp.float32)
    mixed = jnp.sum(picked.reshape(tok_count, 2, -1) * gates[:, :, None], axis=1)
    return mixed.astype(jnp.bfloat16)


def solution(mesh):
    placed = (
        P(("dp", "seq"), "expert"),
        P(("dp", "seq"), "expert"),
        P(("dp", "seq"), "expert"),
        P("dp"),
        P(("dp", "seq", "expert"), None),
        P(("dp", "seq", "expert"), None),
        P("expert", None, "seq"),
    )
    return jax.shard_map(
        shards,
        mesh=mesh,
        in_specs=placed,
        out_specs=P(("dp", "seq", "expert"), None),
        check_vma=False,
    )
```

```python
import functools

import jax
import jax.numpy as jnp
from jax import lax
from jax.experimental import pallas as pl
from jax.experimental.pallas import tpu as pltpu
from jax.sharding import PartitionSpec as P

HD = 128
LONGEST = 1024
F32 = jnp.float32
BF16 = jnp.bfloat16
VMEM = pl.BlockSpec(memory_space=pltpu.VMEM)


def exchange(x, axis):
    return lax.all_to_all(x, axis, split_axis=0, concat_axis=0, tiled=True)


def attend(seq_count, begin_ref, routes_ref, q_ref, *refs):
    parts, out_ref = refs[:-1], refs[-1]
    heads, q_rows, _ = q_ref.shape
    shard_len = parts[0].shape[1]
    me = lax.axis_index("seq")
    rows = heads * q_rows
    queries = q_ref[...].reshape(rows, HD)
    begin = begin_ref[...]
    place = lax.broadcasted_iota(jnp.int32, (rows, 1), 0) % q_rows
    qpos = (me + 1) * shard_len - q_rows + place
    scores = []
    for d, part in enumerate(parts):
        count = part.shape[1]
        kpos = (me + 1 - d) * shard_len - count + lax.broadcasted_iota(jnp.int32, (1, count), 1)
        score = lax.dot_general(
            queries, part[0], (((1,), (1,)), ((), ())), preferred_element_type=F32
        )
        allowed = kpos >= begin
        if d == 0:
            allowed = allowed & (kpos <= qpos)
        scores.append(jnp.where(allowed, score, F32(-1e30)))
    peak = functools.reduce(jnp.maximum, [jnp.max(s, axis=1, keepdims=True) for s in scores])
    total = jnp.zeros((rows, 1), F32)
    acc = jnp.zeros((rows, HD), F32)
    for score, part in zip(scores, parts):
        weight = jnp.exp((score - peak) * F32(HD**-0.5))
        total = total + jnp.sum(weight, axis=1, keepdims=True)
        acc = acc + jnp.dot(weight.astype(BF16), part[1], preferred_element_type=F32)
    attended = (acc / total).astype(BF16)
    wide = jnp.concatenate([attended[h * q_rows : (h + 1) * q_rows] for h in range(heads)], axis=1)

    blocks, _, tokens = routes_ref.shape
    experts = out_ref.shape[0] // seq_count
    slots = out_ref.shape[1]
    capacity = slots // blocks
    spread = lax.broadcasted_iota(jnp.int32, (tokens, q_rows), 0) == (
        lax.broadcasted_iota(jnp.int32, (tokens, q_rows), 1) % tokens
    )
    block_of = lax.broadcasted_iota(jnp.int32, (blocks, q_rows), 1) // tokens
    in_block = lax.broadcasted_iota(jnp.int32, (blocks, q_rows), 0) == block_of
    expert_id = lax.broadcasted_iota(jnp.int32, (experts, q_rows), 0).astype(F32)
    named = jnp.zeros((experts, q_rows), jnp.bool_)
    for k in range(2):
        chosen = routes_ref[:, k, :].astype(F32).astype(BF16)
        by_block = jnp.dot(chosen, spread.astype(BF16), preferred_element_type=F32)
        flat = jnp.sum(jnp.where(in_block, by_block, 0.0), axis=0, keepdims=True)
        named = named | (flat == expert_id)
    r = lax.broadcasted_iota(jnp.int32, (q_rows, q_rows), 0)
    c = lax.broadcasted_iota(jnp.int32, (q_rows, q_rows), 1)
    earlier = (r // tokens == c // tokens) & (r < c)
    ahead = jnp.dot(named.astype(BF16), earlier.astype(BF16), preferred_element_type=F32)
    token_block = lax.broadcasted_iota(jnp.int32, (experts, q_rows), 1) // tokens
    slot = jnp.where(named, ahead + (token_block * capacity).astype(F32), F32(-1))
    slot_id = lax.broadcasted_iota(jnp.int32, (slots, q_rows), 0).astype(F32)
    selector = jnp.concatenate(
        [(slot_id == slot[e : e + 1, :]).astype(F32) for e in range(experts)], axis=0
    ).astype(BF16)
    picked = jnp.dot(selector, wide, preferred_element_type=F32)
    picked = picked.reshape(experts, slots, picked.shape[1]).astype(BF16)
    for s in range(seq_count):
        out_ref[s * experts : (s + 1) * experts] = picked


def project(experts, x_ref, w_ref, out_ref, w_vmem, sems):
    chunk = x_ref.shape[2]
    seq_count = x_ref.shape[0] // experts
    slots = x_ref.shape[1]
    rows = seq_count * slots

    def copy(e):
        at = pl.ds(e * chunk, chunk)
        return pltpu.make_async_copy(w_ref.at[0, at], w_vmem.at[at], sems.at[e])

    for e in range(experts):
        copy(e).start()
    acc = jnp.zeros((rows, w_ref.shape[2]), F32)
    square = jnp.zeros((rows, 1), F32)
    for e in range(experts):
        x = jnp.concatenate([x_ref[s * experts + e].astype(F32) for s in range(seq_count)], axis=0)
        square = square + jnp.sum(x * x, axis=1, keepdims=True)
        copy(e).wait()
        acc = acc + jnp.dot(
            x.astype(BF16), w_vmem[e * chunk : (e + 1) * chunk], preferred_element_type=F32
        )
    upper = acc * lax.rsqrt(square / F32(experts * chunk) + F32(1e-05))
    out_ref[...] = (upper / (1.0 + jnp.exp(-upper))).astype(BF16)


def mix(back_ref, selector_ref, gates_ref, out_ref):
    tokens = gates_ref.shape[0] // 2
    units = back_ref.shape[2]
    for s in range(back_ref.shape[0]):
        rows = jnp.dot(selector_ref[...], back_ref[s], preferred_element_type=F32)
        rows = rows * gates_ref[:, :1]
        out_ref[:, s * units : (s + 1) * units] = (rows[:tokens] + rows[tokens:]).astype(BF16)


def shards(queries, keys, values, lengths, routes, gates, w_up):
    q_rows, width = queries.shape
    shard_len = keys.shape[0]
    seq_count = lax.axis_size("seq")
    expert_count = lax.axis_size("expert")
    capacity = 3
    tok_count = routes.shape[0]
    per_expert = expert_count * capacity
    reach = -(-(LONGEST - 1) // shard_len)

    kv_own = jnp.concatenate([keys, values], axis=0).reshape(2, shard_len, HD)
    ring = [[(i, (i + d) % seq_count) for i in range(seq_count)] for d in range(reach + 1)]
    last = lax.ppermute(kv_own[:, shard_len - q_rows :], "seq", ring[reach])
    parts = [kv_own] + [lax.ppermute(kv_own, "seq", ring[d]) for d in range(1, reach)] + [last]
    row_routes = exchange(
        jnp.broadcast_to(routes.T[None], (expert_count, 2, tok_count)), "expert"
    )

    heads = width // HD
    q_heads = queries.reshape(q_rows, heads, HD).transpose(1, 0, 2)
    starts = jnp.cumsum(lengths) - lengths
    rows = jnp.arange(heads * q_rows, dtype=jnp.int32)[:, None]
    qpos = (lax.axis_index("seq") + 1) * shard_len - q_rows + rows % q_rows
    begin = jnp.max(jnp.where(starts[None, :] <= qpos, starts[None, :], 0), axis=1, keepdims=True)

    flat = routes.T.reshape(-1)
    token = jnp.arange(2 * tok_count, dtype=jnp.int32) % tok_count
    before = (flat[:, None] == flat[None, :]) & (token[:, None] > token[None, :])
    own_target = flat * capacity + jnp.sum(before.astype(jnp.int32), axis=1)
    own_selector = (
        own_target[:, None] == jnp.arange(per_expert, dtype=jnp.int32)[None, :]
    ).astype(BF16)

    outgoing = pl.pallas_call(
        functools.partial(attend, seq_count),
        out_shape=jax.ShapeDtypeStruct((seq_count * expert_count, per_expert, width), BF16),
        in_specs=[VMEM] * (3 + len(parts)),
        out_specs=VMEM,
        compiler_params=pltpu.CompilerParams(vmem_limit_bytes=24 << 20),
        name="attend",
    )(begin, row_routes, q_heads, *parts)
    gate_rows = jnp.broadcast_to(gates.T.reshape(-1, 1), (2 * tok_count, HD))
    outgoing, own_selector, gate_rows = lax.optimization_barrier(
        (outgoing, own_selector, gate_rows)
    )
    landed = exchange(outgoing, ("seq", "expert"))
    act = pl.pallas_call(
        functools.partial(project, expert_count),
        out_shape=jax.ShapeDtypeStruct((seq_count * per_expert, w_up.shape[2]), BF16),
        in_specs=[VMEM, pl.BlockSpec(memory_space=pltpu.HBM)],
        out_specs=VMEM,
        scratch_shapes=[
            pltpu.VMEM(w_up.shape[1:], BF16),
            pltpu.SemaphoreType.DMA((expert_count,)),
        ],
        compiler_params=pltpu.CompilerParams(vmem_limit_bytes=32 << 20),
        name="project",
    )(landed, pltpu.with_memory_space_constraint(w_up, pltpu.HBM))
    ff_local = act.shape[1]
    back = exchange(act.reshape(seq_count * expert_count, capacity, ff_local), ("seq", "expert"))
    back = back.reshape(seq_count, per_expert, ff_local)
    return pl.pallas_call(
        mix,
        out_shape=jax.ShapeDtypeStruct((tok_count, seq_count * ff_local), BF16),
        in_specs=[VMEM] * 3,
        out_specs=VMEM,
        compiler_params=pltpu.CompilerParams(vmem_limit_bytes=16 << 20),
        name="mix",
    )(back, own_selector, gate_rows)


def solution(mesh):
    placed = (
        P(("dp", "seq"), "expert"),
        P(("dp", "seq"), "expert"),
        P(("dp", "seq"), "expert"),
        P("dp"),
        P(("dp", "seq", "expert"), None),
        P(("dp", "seq", "expert"), None),
        P("expert", None, "seq"),
    )
    return jax.shard_map(
        shards,
        mesh=mesh,
        in_specs=placed,
        out_specs=P(("dp", "seq", "expert"), None),
        check_vma=False,
    )
```

```python
import functools

import jax
import jax.numpy as jnp
from jax import lax
from jax.experimental import pallas as pl
from jax.experimental.pallas import tpu as pltpu
from jax.sharding import PartitionSpec as P

HD = 128
LONGEST = 1024
FIXED = 32767
DIGITS = 8192
F32 = jnp.float32
BF16 = jnp.bfloat16
VMEM = pl.BlockSpec(memory_space=pltpu.VMEM)


def exchange(x, axis):
    return lax.all_to_all(x, axis, split_axis=0, concat_axis=0, tiled=True)


def attend(begin_ref, routes_ref, q_ref, *refs):
    parts, out_ref = refs[:-1], refs[-1]
    heads, q_rows, _ = q_ref.shape
    shard_len = parts[0].shape[1]
    me = lax.axis_index("seq")
    rows = heads * q_rows
    queries = q_ref[...].reshape(rows, HD)
    begin = begin_ref[...]
    place = lax.broadcasted_iota(jnp.int32, (rows, 1), 0) % q_rows
    qpos = (me + 1) * shard_len - q_rows + place
    scores = []
    for d, part in enumerate(parts):
        count = part.shape[1]
        kpos = (me + 1 - d) * shard_len - count + lax.broadcasted_iota(jnp.int32, (1, count), 1)
        score = lax.dot_general(
            queries, part[0], (((1,), (1,)), ((), ())), preferred_element_type=F32
        )
        allowed = kpos >= begin
        if d == 0:
            allowed = allowed & (kpos <= qpos)
        scores.append(jnp.where(allowed, score, F32(-1e30)))
    peak = functools.reduce(jnp.maximum, [jnp.max(s, axis=1, keepdims=True) for s in scores])
    total = jnp.zeros((rows, 1), F32)
    acc = jnp.zeros((rows, HD), F32)
    for score, part in zip(scores, parts):
        weight = jnp.exp((score - peak) * F32(HD**-0.5))
        total = total + jnp.sum(weight, axis=1, keepdims=True)
        acc = acc + jnp.dot(weight.astype(BF16), part[1], preferred_element_type=F32)
    attended = (acc / total).astype(BF16)
    wide = jnp.concatenate([attended[h * q_rows : (h + 1) * q_rows] for h in range(heads)], axis=1)

    blocks, _, tokens = routes_ref.shape
    experts = out_ref.shape[0]
    slots = out_ref.shape[1]
    capacity = slots // blocks
    spread = lax.broadcasted_iota(jnp.int32, (tokens, q_rows), 0) == (
        lax.broadcasted_iota(jnp.int32, (tokens, q_rows), 1) % tokens
    )
    block_of = lax.broadcasted_iota(jnp.int32, (blocks, q_rows), 1) // tokens
    in_block = lax.broadcasted_iota(jnp.int32, (blocks, q_rows), 0) == block_of
    expert_id = lax.broadcasted_iota(jnp.int32, (experts, q_rows), 0).astype(F32)
    named = jnp.zeros((experts, q_rows), jnp.bool_)
    for k in range(2):
        chosen = routes_ref[:, k, :].astype(F32).astype(BF16)
        by_block = jnp.dot(chosen, spread.astype(BF16), preferred_element_type=F32)
        flat = jnp.sum(jnp.where(in_block, by_block, 0.0), axis=0, keepdims=True)
        named = named | (flat == expert_id)
    r = lax.broadcasted_iota(jnp.int32, (q_rows, q_rows), 0)
    c = lax.broadcasted_iota(jnp.int32, (q_rows, q_rows), 1)
    earlier = (r // tokens == c // tokens) & (r < c)
    ahead = jnp.dot(named.astype(BF16), earlier.astype(BF16), preferred_element_type=F32)
    token_block = lax.broadcasted_iota(jnp.int32, (experts, q_rows), 1) // tokens
    slot = jnp.where(named, ahead + (token_block * capacity).astype(F32), F32(-1))
    slot_id = lax.broadcasted_iota(jnp.int32, (slots, q_rows), 0).astype(F32)
    selector = jnp.concatenate(
        [(slot_id == slot[e : e + 1, :]).astype(F32) for e in range(experts)], axis=0
    ).astype(BF16)
    picked = jnp.dot(selector, wide, preferred_element_type=F32)
    out_ref[...] = picked.reshape(out_ref.shape).astype(BF16)


def pack(x_ref, out_ref):
    experts, _, chunk = x_ref.shape
    parts = [x_ref[e].astype(F32) for e in range(experts)]
    square = sum(jnp.sum(x * x, axis=1, keepdims=True) for x in parts)
    largest = functools.reduce(
        jnp.maximum, [jnp.max(jnp.abs(x), axis=1, keepdims=True) for x in parts]
    )
    largest = jnp.maximum(largest, F32(1e-30))
    up = F32(FIXED) / largest
    for e, x in enumerate(parts):
        fixed = jnp.round(x * up).astype(jnp.int32)
        out_ref[:, e * chunk : (e + 1) * chunk] = fixed.astype(jnp.int16)
    down = largest * F32(1 / FIXED) * lax.rsqrt(square / F32(experts * chunk) + F32(1e-05))
    power = jnp.floor(jnp.log2(down))
    digits = jnp.round(down * jnp.exp2(-power) * F32(DIGITS))
    tail = (x_ref.shape[1], out_ref.shape[1] - experts * chunk)
    lane = lax.broadcasted_iota(jnp.int32, tail, 1)
    factor = jnp.where(lane == 0, digits, jnp.where(lane == 1, power, F32(0)))
    out_ref[:, experts * chunk :] = factor.astype(jnp.int32).astype(jnp.int16)


def project(chunks, x_ref, w_ref, out_ref, w_vmem, sems):
    seq_count = x_ref.shape[0]
    depth = w_vmem.shape[0]
    chunk = depth // chunks

    def copy(e):
        at = pl.ds(e * chunk, chunk)
        return pltpu.make_async_copy(w_ref.at[0, at], w_vmem.at[at], sems.at[e])

    def rows(lo, size):
        part = [x_ref[s, :, lo : lo + size].astype(jnp.int32) for s in range(seq_count)]
        return jnp.concatenate(part, axis=0).astype(F32)

    for e in range(chunks):
        copy(e).start()
    factor = rows(depth, HD)
    factor = factor[:, 0:1] * F32(1 / DIGITS) * jnp.exp2(factor[:, 1:2])
    acc = jnp.zeros(out_ref.shape, F32)
    for e in range(chunks):
        x = rows(e * chunk, chunk).astype(BF16)
        copy(e).wait()
        acc = acc + jnp.dot(
            x, w_vmem[e * chunk : (e + 1) * chunk], preferred_element_type=F32
        )
    upper = acc * factor
    out_ref[...] = (upper / (1.0 + jnp.exp(-upper))).astype(BF16)


def mix(back_ref, selector_ref, gates_ref, out_ref):
    tokens = gates_ref.shape[0] // 2
    units = back_ref.shape[2]
    for s in range(back_ref.shape[0]):
        rows = jnp.dot(selector_ref[...], back_ref[s], preferred_element_type=F32)
        rows = rows * gates_ref[:, :1]
        out_ref[:, s * units : (s + 1) * units] = (rows[:tokens] + rows[tokens:]).astype(BF16)


def shards(queries, keys, values, lengths, routes, gates, w_up):
    q_rows, width = queries.shape
    shard_len = keys.shape[0]
    seq_count = lax.axis_size("seq")
    expert_count = lax.axis_size("expert")
    capacity = 3
    tok_count = routes.shape[0]
    per_expert = expert_count * capacity
    reach = -(-(LONGEST - 1) // shard_len)

    kv_own = jnp.concatenate([keys, values], axis=0).reshape(2, shard_len, HD)
    ring = [[(i, (i + d) % seq_count) for i in range(seq_count)] for d in range(reach + 1)]
    last = lax.ppermute(kv_own[:, shard_len - q_rows :], "seq", ring[reach])
    parts = [kv_own] + [lax.ppermute(kv_own, "seq", ring[d]) for d in range(1, reach)] + [last]
    row_routes = exchange(
        jnp.broadcast_to(routes.T[None], (expert_count, 2, tok_count)), "expert"
    )

    heads = width // HD
    q_heads = queries.reshape(q_rows, heads, HD).transpose(1, 0, 2)
    starts = jnp.cumsum(lengths) - lengths
    rows = jnp.arange(heads * q_rows, dtype=jnp.int32)[:, None]
    qpos = (lax.axis_index("seq") + 1) * shard_len - q_rows + rows % q_rows
    begin = jnp.max(jnp.where(starts[None, :] <= qpos, starts[None, :], 0), axis=1, keepdims=True)

    flat = routes.T.reshape(-1)
    token = jnp.arange(2 * tok_count, dtype=jnp.int32) % tok_count
    before = (flat[:, None] == flat[None, :]) & (token[:, None] > token[None, :])
    own_target = flat * capacity + jnp.sum(before.astype(jnp.int32), axis=1)
    own_selector = (
        own_target[:, None] == jnp.arange(per_expert, dtype=jnp.int32)[None, :]
    ).astype(BF16)

    outgoing = pl.pallas_call(
        attend,
        out_shape=jax.ShapeDtypeStruct((expert_count, per_expert, width), BF16),
        in_specs=[VMEM] * (3 + len(parts)),
        out_specs=VMEM,
        compiler_params=pltpu.CompilerParams(vmem_limit_bytes=24 << 20),
        name="attend",
    )(begin, row_routes, q_heads, *parts)
    gate_rows = jnp.broadcast_to(gates.T.reshape(-1, 1), (2 * tok_count, HD))
    outgoing, own_selector, gate_rows = lax.optimization_barrier(
        (outgoing, own_selector, gate_rows)
    )
    landed = exchange(outgoing, "expert")
    packed = pl.pallas_call(
        pack,
        out_shape=jax.ShapeDtypeStruct((per_expert, expert_count * width + HD), jnp.int16),
        in_specs=[VMEM],
        out_specs=VMEM,
        compiler_params=pltpu.CompilerParams(vmem_limit_bytes=16 << 20),
        name="pack",
    )(landed)
    incoming = lax.all_gather(packed, "seq")
    act = pl.pallas_call(
        functools.partial(project, expert_count),
        out_shape=jax.ShapeDtypeStruct((seq_count * per_expert, w_up.shape[2]), BF16),
        in_specs=[VMEM, pl.BlockSpec(memory_space=pltpu.HBM)],
        out_specs=VMEM,
        scratch_shapes=[
            pltpu.VMEM(w_up.shape[1:], BF16),
            pltpu.SemaphoreType.DMA((expert_count,)),
        ],
        compiler_params=pltpu.CompilerParams(vmem_limit_bytes=32 << 20),
        name="project",
    )(incoming, pltpu.with_memory_space_constraint(w_up, pltpu.HBM))
    ff_local = act.shape[1]
    back = exchange(act.reshape(seq_count * expert_count, capacity, ff_local), ("seq", "expert"))
    back = back.reshape(seq_count, per_expert, ff_local)
    return pl.pallas_call(
        mix,
        out_shape=jax.ShapeDtypeStruct((tok_count, seq_count * ff_local), BF16),
        in_specs=[VMEM] * 3,
        out_specs=VMEM,
        compiler_params=pltpu.CompilerParams(vmem_limit_bytes=16 << 20),
        name="mix",
    )(back, own_selector, gate_rows)


def solution(mesh):
    placed = (
        P(("dp", "seq"), "expert"),
        P(("dp", "seq"), "expert"),
        P(("dp", "seq"), "expert"),
        P("dp"),
        P(("dp", "seq", "expert"), None),
        P(("dp", "seq", "expert"), None),
        P("expert", None, "seq"),
    )
    return jax.shard_map(
        shards,
        mesh=mesh,
        in_specs=placed,
        out_specs=P(("dp", "seq", "expert"), None),
        check_vma=False,
    )
```

```python
import functools

import jax
import jax.numpy as jnp
from jax import lax
from jax.experimental import pallas as pl
from jax.experimental.pallas import tpu as pltpu
from jax.sharding import PartitionSpec as P

HD = 128
LONGEST = 1024
FIXED = 32767
DIGITS = 8192
F32 = jnp.float32
BF16 = jnp.bfloat16
VMEM = pl.BlockSpec(memory_space=pltpu.VMEM)


def exchange(x, axis):
    return lax.all_to_all(x, axis, split_axis=0, concat_axis=0, tiled=True)


def fetch(pairs, sems):
    copies = [pltpu.make_async_copy(a, b, sems.at[i]) for i, (a, b) in enumerate(pairs)]
    for copy in copies:
        copy.start()
    for copy in copies:
        copy.wait()


def first(keys_ref, values_ref, routes_ref, kv_ref, last_ref, message_ref, routes_vmem, sems):
    shard_len, q_rows = keys_ref.shape[0], last_ref.shape[1]
    end = pl.ds(shard_len - q_rows, q_rows)
    pairs = [
        (keys_ref, kv_ref.at[0]),
        (values_ref, kv_ref.at[1]),
        (keys_ref.at[end], last_ref.at[0]),
        (values_ref.at[end], last_ref.at[1]),
        (routes_ref, routes_vmem),
    ]
    fetch(pairs, sems)
    message_ref[...] = jnp.broadcast_to(routes_vmem[...][None], message_ref.shape)


def second(
    shard_len,
    q_hbm, lengths_hbm, routes_hbm, gates_hbm,
    heads_ref, begin_ref, selector_ref, column_ref,
    q_ref, lengths_ref, routes_ref, gates_ref, sems,
):
    pairs = [
        (q_hbm, q_ref),
        (lengths_hbm, lengths_ref),
        (routes_hbm, routes_ref),
        (gates_hbm, gates_ref),
    ]
    fetch(pairs, sems)
    heads, q_rows, _ = heads_ref.shape
    for h in range(heads):
        heads_ref[h] = q_ref[:, h * HD : (h + 1) * HD]
    routes = routes_ref[...]
    place = lax.broadcasted_iota(jnp.int32, begin_ref.shape, 0)
    qpos = (lax.axis_index("seq") + 1) * shard_len - q_rows + place
    begin = jnp.zeros(begin_ref.shape, jnp.int32)
    start = jnp.zeros((1, 1), jnp.int32)
    for j in range(lengths_ref.shape[1]):
        begin = jnp.where(start <= qpos, start, begin)
        start = start + lengths_ref[:, j : j + 1]
    begin_ref[...] = begin

    _, rows, tokens = selector_ref.shape
    capacity = 3
    row = lax.broadcasted_iota(jnp.int32, (rows, tokens), 0)
    named = [routes[k : k + 1, :] == row // capacity for k in range(2)]
    before = lax.broadcasted_iota(jnp.int32, (tokens, tokens), 0) < (
        lax.broadcasted_iota(jnp.int32, (tokens, tokens), 1)
    )
    either = (named[0] | named[1]).astype(F32).astype(BF16)
    ahead = jnp.dot(either, before.astype(F32).astype(BF16), preferred_element_type=F32)
    right = ahead == (row % capacity).astype(F32)
    diagonal = lax.broadcasted_iota(jnp.int32, (tokens, tokens), 0) == (
        lax.broadcasted_iota(jnp.int32, (tokens, tokens), 1)
    )
    for k in range(2):
        selector_ref[k] = (named[k] & right).astype(F32).astype(BF16)
        gate = jnp.where(diagonal, gates_ref[k : k + 1, :], F32(0))
        gate = jnp.sum(gate, axis=1, keepdims=True)
        column_ref[k] = jnp.broadcast_to(gate, column_ref.shape[1:])


def attend(begin_ref, routes_ref, q_ref, *refs):
    parts, out_ref = refs[:-1], refs[-1]
    heads, q_rows, _ = q_ref.shape
    shard_len = parts[0].shape[1]
    me = lax.axis_index("seq")
    rows = heads * q_rows
    queries = q_ref[...].reshape(rows, HD)
    begin = jnp.concatenate([begin_ref[:, 0:1]] * heads, axis=0)
    place = lax.broadcasted_iota(jnp.int32, (rows, 1), 0) % q_rows
    qpos = (me + 1) * shard_len - q_rows + place
    scores = []
    for d, part in enumerate(parts):
        count = part.shape[1]
        kpos = (me + 1 - d) * shard_len - count + lax.broadcasted_iota(jnp.int32, (1, count), 1)
        score = lax.dot_general(
            queries, part[0], (((1,), (1,)), ((), ())), preferred_element_type=F32
        )
        allowed = kpos >= begin
        if d == 0:
            allowed = allowed & (kpos <= qpos)
        scores.append(jnp.where(allowed, score, F32(-1e30)))
    peak = functools.reduce(jnp.maximum, [jnp.max(s, axis=1, keepdims=True) for s in scores])
    total = jnp.zeros((rows, 1), F32)
    acc = jnp.zeros((rows, HD), F32)
    for score, part in zip(scores, parts):
        weight = jnp.exp((score - peak) * F32(HD**-0.5))
        total = total + jnp.sum(weight, axis=1, keepdims=True)
        acc = acc + jnp.dot(weight.astype(BF16), part[1], preferred_element_type=F32)
    attended = (acc / total).astype(BF16)
    wide = jnp.concatenate([attended[h * q_rows : (h + 1) * q_rows] for h in range(heads)], axis=1)

    blocks, _, tokens = routes_ref.shape
    experts = out_ref.shape[0]
    slots = out_ref.shape[1]
    capacity = slots // blocks
    spread = lax.broadcasted_iota(jnp.int32, (tokens, q_rows), 0) == (
        lax.broadcasted_iota(jnp.int32, (tokens, q_rows), 1) % tokens
    )
    block_of = lax.broadcasted_iota(jnp.int32, (blocks, q_rows), 1) // tokens
    in_block = lax.broadcasted_iota(jnp.int32, (blocks, q_rows), 0) == block_of
    expert_id = lax.broadcasted_iota(jnp.int32, (experts, q_rows), 0).astype(F32)
    named = jnp.zeros((experts, q_rows), jnp.bool_)
    for k in range(2):
        chosen = routes_ref[:, k, :].astype(F32).astype(BF16)
        by_block = jnp.dot(chosen, spread.astype(BF16), preferred_element_type=F32)
        flat = jnp.sum(jnp.where(in_block, by_block, 0.0), axis=0, keepdims=True)
        named = named | (flat == expert_id)
    r = lax.broadcasted_iota(jnp.int32, (q_rows, q_rows), 0)
    c = lax.broadcasted_iota(jnp.int32, (q_rows, q_rows), 1)
    earlier = (r // tokens == c // tokens) & (r < c)
    ahead = jnp.dot(named.astype(BF16), earlier.astype(BF16), preferred_element_type=F32)
    token_block = lax.broadcasted_iota(jnp.int32, (experts, q_rows), 1) // tokens
    slot = jnp.where(named, ahead + (token_block * capacity).astype(F32), F32(-1))
    slot_id = lax.broadcasted_iota(jnp.int32, (slots, q_rows), 0).astype(F32)
    selector = jnp.concatenate(
        [(slot_id == slot[e : e + 1, :]).astype(F32) for e in range(experts)], axis=0
    ).astype(BF16)
    picked = jnp.dot(selector, wide, preferred_element_type=F32)
    out_ref[...] = picked.reshape(out_ref.shape).astype(BF16)


def pack(x_ref, out_ref):
    experts, _, chunk = x_ref.shape
    parts = [x_ref[e].astype(F32) for e in range(experts)]
    square = sum(jnp.sum(x * x, axis=1, keepdims=True) for x in parts)
    largest = functools.reduce(
        jnp.maximum, [jnp.max(jnp.abs(x), axis=1, keepdims=True) for x in parts]
    )
    largest = jnp.maximum(largest, F32(1e-30))
    up = F32(FIXED) / largest
    for e, x in enumerate(parts):
        fixed = jnp.round(x * up).astype(jnp.int32)
        out_ref[:, e * chunk : (e + 1) * chunk] = fixed.astype(jnp.int16)
    down = largest * F32(1 / FIXED) * lax.rsqrt(square / F32(experts * chunk) + F32(1e-05))
    power = jnp.floor(jnp.log2(down))
    digits = jnp.round(down * jnp.exp2(-power) * F32(DIGITS))
    tail = (x_ref.shape[1], out_ref.shape[1] - experts * chunk)
    lane = lax.broadcasted_iota(jnp.int32, tail, 1)
    factor = jnp.where(lane == 0, digits, jnp.where(lane == 1, power, F32(0)))
    out_ref[:, experts * chunk :] = factor.astype(jnp.int32).astype(jnp.int16)


def project(chunks, x_ref, w_ref, out_ref, w_vmem, sems):
    seq_count = x_ref.shape[0]
    depth = w_vmem.shape[0]
    chunk = depth // chunks

    def copy(e):
        at = pl.ds(e * chunk, chunk)
        return pltpu.make_async_copy(w_ref.at[0, at], w_vmem.at[at], sems.at[e])

    def rows(lo, size):
        part = [x_ref[s, :, lo : lo + size].astype(jnp.int32) for s in range(seq_count)]
        return jnp.concatenate(part, axis=0).astype(F32)

    for e in range(chunks):
        copy(e).start()
    factor = rows(depth, HD)
    factor = factor[:, 0:1] * F32(1 / DIGITS) * jnp.exp2(factor[:, 1:2])
    acc = jnp.zeros(out_ref.shape, F32)
    for e in range(chunks):
        x = rows(e * chunk, chunk).astype(BF16)
        copy(e).wait()
        acc = acc + jnp.dot(
            x, w_vmem[e * chunk : (e + 1) * chunk], preferred_element_type=F32
        )
    upper = acc * factor
    out_ref[...] = (upper / (1.0 + jnp.exp(-upper))).astype(BF16)


def mix(back_ref, selector_ref, column_ref, out_ref):
    units = back_ref.shape[2]
    for s in range(back_ref.shape[0]):
        both = F32(0)
        for k in range(2):
            rows = lax.dot_general(
                selector_ref[k],
                back_ref[s],
                (((0,), (0,)), ((), ())),
                preferred_element_type=F32,
            )
            both = both + rows * column_ref[k, :, 0:1]
        out_ref[:, s * units : (s + 1) * units] = both.astype(BF16)


def shards(queries, keys, values, lengths, routes, gates, w_up):
    q_rows, width = queries.shape
    shard_len = keys.shape[0]
    seq_count = lax.axis_size("seq")
    expert_count = lax.axis_size("expert")
    capacity = 3
    tok_count = routes.shape[0]
    per_expert = expert_count * capacity
    reach = -(-(LONGEST - 1) // shard_len)

    heads = width // HD
    keys, values, queries, lengths, routes, gates = (
        pltpu.with_memory_space_constraint(x, pltpu.HBM)
        for x in (keys, values, queries, lengths.reshape(1, -1), routes.T, gates.T)
    )
    hbm = pl.BlockSpec(memory_space=pltpu.HBM)
    kv_own, kv_last, message = pl.pallas_call(
        first,
        out_shape=(
            jax.ShapeDtypeStruct((2, shard_len, HD), BF16),
            jax.ShapeDtypeStruct((2, q_rows, HD), BF16),
            jax.ShapeDtypeStruct((expert_count, 2, tok_count), jnp.int32),
        ),
        in_specs=[hbm] * 3,
        out_specs=(VMEM,) * 3,
        scratch_shapes=[
            pltpu.VMEM(routes.shape, jnp.int32),
            pltpu.SemaphoreType.DMA((5,)),
        ],
        compiler_params=pltpu.CompilerParams(vmem_limit_bytes=8 << 20),
        name="first",
    )(keys, values, routes)
    q_heads, begin, selectors, columns = pl.pallas_call(
        functools.partial(second, shard_len),
        out_shape=(
            jax.ShapeDtypeStruct((heads, q_rows, HD), BF16),
            jax.ShapeDtypeStruct((q_rows, HD), jnp.int32),
            jax.ShapeDtypeStruct((2, per_expert, tok_count), BF16),
            jax.ShapeDtypeStruct((2, tok_count, HD), F32),
        ),
        in_specs=[hbm] * 4,
        out_specs=(VMEM,) * 4,
        scratch_shapes=[
            pltpu.VMEM(queries.shape, BF16),
            pltpu.VMEM(lengths.shape, jnp.int32),
            pltpu.VMEM(routes.shape, jnp.int32),
            pltpu.VMEM(gates.shape, F32),
            pltpu.SemaphoreType.DMA((4,)),
        ],
        compiler_params=pltpu.CompilerParams(vmem_limit_bytes=8 << 20),
        cost_estimate=pl.CostEstimate(flops=4_000_000, bytes_accessed=200_000, transcendentals=0),
        name="second",
    )(queries, lengths, routes, gates)
    ring = [[(i, (i + d) % seq_count) for i in range(seq_count)] for d in range(reach + 1)]
    last = lax.ppermute(kv_last, "seq", ring[reach])
    parts = [kv_own] + [lax.ppermute(kv_own, "seq", ring[d]) for d in range(1, reach)] + [last]
    row_routes = exchange(message, "expert")

    outgoing = pl.pallas_call(
        attend,
        out_shape=jax.ShapeDtypeStruct((expert_count, per_expert, width), BF16),
        in_specs=[VMEM] * (3 + len(parts)),
        out_specs=VMEM,
        compiler_params=pltpu.CompilerParams(vmem_limit_bytes=24 << 20),
        name="attend",
    )(begin, row_routes, q_heads, *parts)
    landed = exchange(outgoing, "expert")
    packed = pl.pallas_call(
        pack,
        out_shape=jax.ShapeDtypeStruct((per_expert, expert_count * width + HD), jnp.int16),
        in_specs=[VMEM],
        out_specs=VMEM,
        compiler_params=pltpu.CompilerParams(vmem_limit_bytes=16 << 20),
        name="pack",
    )(landed)
    incoming = lax.all_gather(packed, "seq")
    act = pl.pallas_call(
        functools.partial(project, expert_count),
        out_shape=jax.ShapeDtypeStruct((seq_count * per_expert, w_up.shape[2]), BF16),
        in_specs=[VMEM, pl.BlockSpec(memory_space=pltpu.HBM)],
        out_specs=VMEM,
        scratch_shapes=[
            pltpu.VMEM(w_up.shape[1:], BF16),
            pltpu.SemaphoreType.DMA((expert_count,)),
        ],
        compiler_params=pltpu.CompilerParams(vmem_limit_bytes=32 << 20),
        name="project",
    )(incoming, pltpu.with_memory_space_constraint(w_up, pltpu.HBM))
    ff_local = act.shape[1]
    back = exchange(act.reshape(seq_count * expert_count, capacity, ff_local), ("seq", "expert"))
    back = back.reshape(seq_count, per_expert, ff_local)
    return pl.pallas_call(
        mix,
        out_shape=jax.ShapeDtypeStruct((tok_count, seq_count * ff_local), BF16),
        in_specs=[VMEM] * 3,
        out_specs=VMEM,
        compiler_params=pltpu.CompilerParams(vmem_limit_bytes=16 << 20),
        name="mix",
    )(back, selectors, columns)


def solution(mesh):
    placed = (
        P(("dp", "seq"), "expert"),
        P(("dp", "seq"), "expert"),
        P(("dp", "seq"), "expert"),
        P("dp"),
        P(("dp", "seq", "expert"), None),
        P(("dp", "seq", "expert"), None),
        P("expert", None, "seq"),
    )
    return jax.shard_map(
        shards,
        mesh=mesh,
        in_specs=placed,
        out_specs=P(("dp", "seq", "expert"), None),
        check_vma=False,
    )
```

```python
import functools

import jax
import jax.numpy as jnp
from jax import lax
from jax.experimental import pallas as pl
from jax.experimental.pallas import tpu as pltpu
from jax.sharding import PartitionSpec as P


HD = 128
LONGEST = 1024
FIXED = 32767
DIGITS = 8192
F32 = jnp.float32
BF16 = jnp.bfloat16
VMEM = pl.BlockSpec(memory_space=pltpu.VMEM)


def exchange(x, axis):
    return lax.all_to_all(x, axis, split_axis=0, concat_axis=0, tiled=True)


def fetch(pairs, sems):
    copies = [pltpu.make_async_copy(a, b, sems.at[i]) for i, (a, b) in enumerate(pairs)]
    for copy in copies:
        copy.start()
    for copy in copies:
        copy.wait()


def first(keys_ref, values_ref, routes_ref, kv_ref, message_ref, routes_vmem, sems):
    pairs = [
        (keys_ref, kv_ref.at[0]),
        (values_ref, kv_ref.at[1]),
        (routes_ref, routes_vmem),
    ]
    fetch(pairs, sems)
    message_ref[...] = jnp.broadcast_to(routes_vmem[...][None], message_ref.shape)


def forward(near_ref, far_ref, out_ref):
    rows = out_ref.shape[1] - near_ref.shape[1]
    out_ref[:, :rows] = far_ref[:, far_ref.shape[1] - rows :]
    out_ref[:, rows:] = near_ref[...]


def second(
    shard_len,
    q_hbm, lengths_hbm, routes_hbm, gates_hbm,
    heads_ref, begin_ref, selector_ref, column_ref,
    q_ref, lengths_ref, routes_ref, gates_ref, sems,
):
    pairs = [
        (q_hbm, q_ref),
        (lengths_hbm, lengths_ref),
        (routes_hbm, routes_ref),
        (gates_hbm, gates_ref),
    ]
    fetch(pairs, sems)
    heads, q_rows, _ = heads_ref.shape
    for h in range(heads):
        heads_ref[h] = q_ref[:, h * HD : (h + 1) * HD]
    routes = routes_ref[...]
    place = lax.broadcasted_iota(jnp.int32, begin_ref.shape, 0)
    qpos = (lax.axis_index("seq") + 1) * shard_len - q_rows + place
    begin = jnp.zeros(begin_ref.shape, jnp.int32)
    start = jnp.zeros((1, 1), jnp.int32)
    for j in range(lengths_ref.shape[1]):
        begin = jnp.where(start <= qpos, start, begin)
        start = start + lengths_ref[:, j : j + 1]
    begin_ref[...] = begin

    _, rows, tokens = selector_ref.shape
    capacity = 3
    row = lax.broadcasted_iota(jnp.int32, (rows, tokens), 0)
    named = [routes[k : k + 1, :] == row // capacity for k in range(2)]
    before = lax.broadcasted_iota(jnp.int32, (tokens, tokens), 0) < (
        lax.broadcasted_iota(jnp.int32, (tokens, tokens), 1)
    )
    either = (named[0] | named[1]).astype(F32).astype(BF16)
    ahead = jnp.dot(either, before.astype(F32).astype(BF16), preferred_element_type=F32)
    right = ahead == (row % capacity).astype(F32)
    diagonal = lax.broadcasted_iota(jnp.int32, (tokens, tokens), 0) == (
        lax.broadcasted_iota(jnp.int32, (tokens, tokens), 1)
    )
    for k in range(2):
        selector_ref[k] = (named[k] & right).astype(F32).astype(BF16)
        gate = jnp.where(diagonal, gates_ref[k : k + 1, :], F32(0))
        gate = jnp.sum(gate, axis=1, keepdims=True)
        column_ref[k] = jnp.broadcast_to(gate, column_ref.shape[1:])


def attend(begin_ref, routes_ref, q_ref, *refs):
    parts, out_ref = refs[:-1], refs[-1]
    heads, q_rows, _ = q_ref.shape
    shard_len = parts[0].shape[1]
    me = lax.axis_index("seq")
    rows = heads * q_rows
    queries = q_ref[...].reshape(rows, HD)
    begin = jnp.concatenate([begin_ref[:, 0:1]] * heads, axis=0)
    place = lax.broadcasted_iota(jnp.int32, (rows, 1), 0) % q_rows
    qpos = (me + 1) * shard_len - q_rows + place
    scores = []
    for d, part in enumerate(parts):
        count = part.shape[1]
        kpos = (me + 1 - d) * shard_len - count + lax.broadcasted_iota(jnp.int32, (1, count), 1)
        score = lax.dot_general(
            queries, part[0], (((1,), (1,)), ((), ())), preferred_element_type=F32
        )
        allowed = kpos >= begin
        if d == 0:
            allowed = allowed & (kpos <= qpos)
        scores.append(jnp.where(allowed, score, F32(-1e30)))
    peak = functools.reduce(jnp.maximum, [jnp.max(s, axis=1, keepdims=True) for s in scores])
    total = jnp.zeros((rows, 1), F32)
    acc = jnp.zeros((rows, HD), F32)
    for score, part in zip(scores, parts):
        weight = jnp.exp((score - peak) * F32(HD**-0.5))
        total = total + jnp.sum(weight, axis=1, keepdims=True)
        acc = acc + jnp.dot(weight.astype(BF16), part[1], preferred_element_type=F32)
    attended = (acc / total).astype(BF16)
    wide = jnp.concatenate([attended[h * q_rows : (h + 1) * q_rows] for h in range(heads)], axis=1)

    blocks, _, tokens = routes_ref.shape
    experts = out_ref.shape[0]
    slots = out_ref.shape[1]
    capacity = slots // blocks
    spread = lax.broadcasted_iota(jnp.int32, (tokens, q_rows), 0) == (
        lax.broadcasted_iota(jnp.int32, (tokens, q_rows), 1) % tokens
    )
    block_of = lax.broadcasted_iota(jnp.int32, (blocks, q_rows), 1) // tokens
    in_block = lax.broadcasted_iota(jnp.int32, (blocks, q_rows), 0) == block_of
    expert_id = lax.broadcasted_iota(jnp.int32, (experts, q_rows), 0).astype(F32)
    named = jnp.zeros((experts, q_rows), jnp.bool_)
    for k in range(2):
        chosen = routes_ref[:, k, :].astype(F32).astype(BF16)
        by_block = jnp.dot(chosen, spread.astype(BF16), preferred_element_type=F32)
        flat = jnp.sum(jnp.where(in_block, by_block, 0.0), axis=0, keepdims=True)
        named = named | (flat == expert_id)
    r = lax.broadcasted_iota(jnp.int32, (q_rows, q_rows), 0)
    c = lax.broadcasted_iota(jnp.int32, (q_rows, q_rows), 1)
    earlier = (r // tokens == c // tokens) & (r < c)
    ahead = jnp.dot(named.astype(BF16), earlier.astype(BF16), preferred_element_type=F32)
    token_block = lax.broadcasted_iota(jnp.int32, (experts, q_rows), 1) // tokens
    slot = jnp.where(named, ahead + (token_block * capacity).astype(F32), F32(-1))
    slot_id = lax.broadcasted_iota(jnp.int32, (slots, q_rows), 0).astype(F32)
    selector = jnp.concatenate(
        [(slot_id == slot[e : e + 1, :]).astype(F32) for e in range(experts)], axis=0
    ).astype(BF16)
    picked = jnp.dot(selector, wide, preferred_element_type=F32)
    out_ref[...] = picked.reshape(out_ref.shape).astype(BF16)


def pack(x_ref, out_ref):
    experts, _, chunk = x_ref.shape
    parts = [x_ref[e].astype(F32) for e in range(experts)]
    square = sum(jnp.sum(x * x, axis=1, keepdims=True) for x in parts)
    largest = functools.reduce(
        jnp.maximum, [jnp.max(jnp.abs(x), axis=1, keepdims=True) for x in parts]
    )
    largest = jnp.maximum(largest, F32(1e-30))
    up = F32(FIXED) / largest
    for e, x in enumerate(parts):
        fixed = jnp.round(x * up).astype(jnp.int32)
        out_ref[:, e * chunk : (e + 1) * chunk] = fixed.astype(jnp.int16)
    down = largest * F32(1 / FIXED) * lax.rsqrt(square / F32(experts * chunk) + F32(1e-05))
    power = jnp.floor(jnp.log2(down))
    digits = jnp.round(down * jnp.exp2(-power) * F32(DIGITS))
    tail = (x_ref.shape[1], out_ref.shape[1] - experts * chunk)
    lane = lax.broadcasted_iota(jnp.int32, tail, 1)
    factor = jnp.where(lane == 0, digits, jnp.where(lane == 1, power, F32(0)))
    out_ref[:, experts * chunk :] = factor.astype(jnp.int32).astype(jnp.int16)


def project(chunks, x_ref, w_ref, out_ref, w_vmem, sems):
    seq_count = x_ref.shape[0]
    depth = w_vmem.shape[0]
    chunk = depth // chunks

    def copy(e):
        at = pl.ds(e * chunk, chunk)
        return pltpu.make_async_copy(w_ref.at[0, at], w_vmem.at[at], sems.at[e])

    def rows(lo, size):
        part = [x_ref[s, :, lo : lo + size].astype(jnp.int32) for s in range(seq_count)]
        return jnp.concatenate(part, axis=0).astype(F32)

    for e in range(chunks):
        copy(e).start()
    factor = rows(depth, HD)
    factor = factor[:, 0:1] * F32(1 / DIGITS) * jnp.exp2(factor[:, 1:2])
    acc = jnp.zeros(out_ref.shape, F32)
    for e in range(chunks):
        x = rows(e * chunk, chunk).astype(BF16)
        copy(e).wait()
        acc = acc + jnp.dot(
            x, w_vmem[e * chunk : (e + 1) * chunk], preferred_element_type=F32
        )
    upper = acc * factor
    out_ref[...] = (upper / (1.0 + jnp.exp(-upper))).astype(BF16)


def mix(back_ref, selector_ref, column_ref, out_ref):
    units = back_ref.shape[2]
    for s in range(back_ref.shape[0]):
        both = F32(0)
        for k in range(2):
            rows = lax.dot_general(
                selector_ref[k],
                back_ref[s],
                (((0,), (0,)), ((), ())),
                preferred_element_type=F32,
            )
            both = both + rows * column_ref[k, :, 0:1]
        out_ref[:, s * units : (s + 1) * units] = both.astype(BF16)


def shards(queries, keys, values, lengths, routes, gates, w_up):
    q_rows, width = queries.shape
    shard_len = keys.shape[0]
    seq_count = lax.axis_size("seq")
    expert_count = lax.axis_size("expert")
    capacity = 3
    tok_count = routes.shape[0]
    per_expert = expert_count * capacity
    reach = LONGEST + shard_len
    reach = reach - (shard_len - q_rows)

    heads = width // HD
    keys, values, queries, lengths, routes, gates = (
        pltpu.with_memory_space_constraint(x, pltpu.HBM)
        for x in (keys, values, queries, lengths.reshape(1, -1), routes.T, gates.T)
    )
    hbm = pl.BlockSpec(memory_space=pltpu.HBM)
    kv_own, message = pl.pallas_call(
        first,
        out_shape=(
            jax.ShapeDtypeStruct((2, shard_len, HD), BF16),
            jax.ShapeDtypeStruct((expert_count, 2, tok_count), jnp.int32),
        ),
        in_specs=[hbm] * 3,
        out_specs=(VMEM,) * 2,
        scratch_shapes=[
            pltpu.VMEM(routes.shape, jnp.int32),
            pltpu.SemaphoreType.DMA((3,)),
        ],
        compiler_params=pltpu.CompilerParams(vmem_limit_bytes=8 << 20),
        name="first",
    )(keys, values, routes)
    q_heads, begin, selectors, columns = pl.pallas_call(
        functools.partial(second, shard_len),
        out_shape=(
            jax.ShapeDtypeStruct((heads, q_rows, HD), BF16),
            jax.ShapeDtypeStruct((q_rows, HD), jnp.int32),
            jax.ShapeDtypeStruct((2, per_expert, tok_count), BF16),
            jax.ShapeDtypeStruct((2, tok_count, HD), F32),
        ),
        in_specs=[hbm] * 4,
        out_specs=(VMEM,) * 4,
        scratch_shapes=[
            pltpu.VMEM(queries.shape, BF16),
            pltpu.VMEM(lengths.shape, jnp.int32),
            pltpu.VMEM(routes.shape, jnp.int32),
            pltpu.VMEM(gates.shape, F32),
            pltpu.SemaphoreType.DMA((4,)),
        ],
        compiler_params=pltpu.CompilerParams(vmem_limit_bytes=8 << 20),
        cost_estimate=pl.CostEstimate(flops=4_000_000, bytes_accessed=200_000, transcendentals=0),
        name="second",
    )(queries, lengths, routes, gates)
    by_one, by_two = ([(i, (i + d) % seq_count) for i in range(seq_count)] for d in (1, 2))
    far = lax.ppermute(kv_own, "seq", by_two)
    near = lax.ppermute(kv_own, "seq", by_one)
    beyond = pl.pallas_call(
        forward,
        out_shape=jax.ShapeDtypeStruct((2, reach - 3 * shard_len, HD), BF16),
        in_specs=[VMEM] * 2,
        out_specs=VMEM,
        compiler_params=pltpu.CompilerParams(vmem_limit_bytes=8 << 20),
        name="forward",
    )(near, far)
    beyond = lax.ppermute(beyond, "seq", by_two)
    parts = [kv_own, near, far, beyond]
    row_routes = exchange(message, "expert")

    outgoing = pl.pallas_call(
        attend,
        out_shape=jax.ShapeDtypeStruct((expert_count, per_expert, width), BF16),
        in_specs=[VMEM] * (3 + len(parts)),
        out_specs=VMEM,
        compiler_params=pltpu.CompilerParams(vmem_limit_bytes=24 << 20),
        name="attend",
    )(begin, row_routes, q_heads, *parts)
    landed = exchange(outgoing, "expert")
    packed = pl.pallas_call(
        pack,
        out_shape=jax.ShapeDtypeStruct((per_expert, expert_count * width + HD), jnp.int16),
        in_specs=[VMEM],
        out_specs=VMEM,
        compiler_params=pltpu.CompilerParams(vmem_limit_bytes=16 << 20),
        name="pack",
    )(landed)
    incoming = lax.all_gather(packed, "seq")
    act = pl.pallas_call(
        functools.partial(project, expert_count),
        out_shape=jax.ShapeDtypeStruct((seq_count * per_expert, w_up.shape[2]), BF16),
        in_specs=[VMEM, pl.BlockSpec(memory_space=pltpu.HBM)],
        out_specs=VMEM,
        scratch_shapes=[
            pltpu.VMEM(w_up.shape[1:], BF16),
            pltpu.SemaphoreType.DMA((expert_count,)),
        ],
        compiler_params=pltpu.CompilerParams(vmem_limit_bytes=32 << 20),
        name="project",
    )(incoming, pltpu.with_memory_space_constraint(w_up, pltpu.HBM))
    ff_local = act.shape[1]
    back = exchange(act.reshape(seq_count * expert_count, capacity, ff_local), ("seq", "expert"))
    back = back.reshape(seq_count, per_expert, ff_local)
    return pl.pallas_call(
        mix,
        out_shape=jax.ShapeDtypeStruct((tok_count, seq_count * ff_local), BF16),
        in_specs=[VMEM] * 3,
        out_specs=VMEM,
        compiler_params=pltpu.CompilerParams(vmem_limit_bytes=16 << 20),
        name="mix",
    )(back, selectors, columns)


def solution(mesh):
    placed = (
        P(("dp", "seq"), "expert"),
        P(("dp", "seq"), "expert"),
        P(("dp", "seq"), "expert"),
        P("dp"),
        P(("dp", "seq", "expert"), None),
        P(("dp", "seq", "expert"), None),
        P("expert", None, "seq"),
    )

    return jax.shard_map(
        shards,
        mesh=mesh,
        in_specs=placed,
        out_specs=P(("dp", "seq", "expert"), None),
        check_vma=False,
    )
```

```python
import functools

import jax
import jax.numpy as jnp
from jax import lax
from jax.experimental import pallas as pl
from jax.experimental.pallas import tpu as pltpu
from jax.sharding import PartitionSpec as P


HD = 128
LONGEST = 1024
FIXED = 32767
DIGITS = 8192
F32 = jnp.float32
BF16 = jnp.bfloat16
VMEM = pl.BlockSpec(memory_space=pltpu.VMEM)


def exchange(x, axis):
    return lax.all_to_all(x, axis, split_axis=0, concat_axis=0, tiled=True)


def fetch(pairs, sems):
    copies = [pltpu.make_async_copy(a, b, sems.at[i]) for i, (a, b) in enumerate(pairs)]
    for copy in copies:
        copy.start()
    for copy in copies:
        copy.wait()


def first(keys_ref, values_ref, routes_ref, kv_ref, message_ref, routes_vmem, sems):
    pairs = [
        (keys_ref, kv_ref.at[0]),
        (values_ref, kv_ref.at[1]),
        (routes_ref, routes_vmem),
    ]
    fetch(pairs, sems)
    message_ref[...] = jnp.broadcast_to(routes_vmem[...][None], message_ref.shape)


def forward(near_ref, far_ref, out_ref):
    rows = out_ref.shape[1] - near_ref.shape[1]
    out_ref[:, :rows] = far_ref[:, far_ref.shape[1] - rows :]
    out_ref[:, rows:] = near_ref[...]


def second(
    shard_len,
    q_hbm, lengths_hbm, routes_hbm, gates_hbm,
    heads_ref, begin_ref, selector_ref, column_ref,
    q_ref, lengths_ref, routes_ref, gates_ref, sems,
):
    pairs = [
        (q_hbm, q_ref),
        (lengths_hbm, lengths_ref),
        (routes_hbm, routes_ref),
        (gates_hbm, gates_ref),
    ]
    fetch(pairs, sems)
    heads, q_rows, _ = heads_ref.shape
    for h in range(heads):
        heads_ref[h] = q_ref[:, h * HD : (h + 1) * HD]
    routes = routes_ref[...]
    place = lax.broadcasted_iota(jnp.int32, begin_ref.shape, 0)
    qpos = (lax.axis_index("seq") + 1) * shard_len - q_rows + place
    begin = jnp.zeros(begin_ref.shape, jnp.int32)
    start = jnp.zeros((1, 1), jnp.int32)
    for j in range(lengths_ref.shape[1]):
        begin = jnp.where(start <= qpos, start, begin)
        start = start + lengths_ref[:, j : j + 1]
    begin_ref[...] = begin

    _, rows, tokens = selector_ref.shape
    capacity = 3
    row = lax.broadcasted_iota(jnp.int32, (rows, tokens), 0)
    named = [routes[k : k + 1, :] == row // capacity for k in range(2)]
    before = lax.broadcasted_iota(jnp.int32, (tokens, tokens), 0) < (
        lax.broadcasted_iota(jnp.int32, (tokens, tokens), 1)
    )
    either = (named[0] | named[1]).astype(F32).astype(BF16)
    ahead = jnp.dot(either, before.astype(F32).astype(BF16), preferred_element_type=F32)
    right = ahead == (row % capacity).astype(F32)
    diagonal = lax.broadcasted_iota(jnp.int32, (tokens, tokens), 0) == (
        lax.broadcasted_iota(jnp.int32, (tokens, tokens), 1)
    )
    for k in range(2):
        selector_ref[k] = (named[k] & right).astype(F32).astype(BF16)
        gate = jnp.where(diagonal, gates_ref[k : k + 1, :], F32(0))
        gate = jnp.sum(gate, axis=1, keepdims=True)
        column_ref[k] = jnp.broadcast_to(gate, column_ref.shape[1:])


def attend(begin_ref, routes_ref, q_ref, *refs):
    parts, out_ref = refs[:-1], refs[-1]
    heads, q_rows, _ = q_ref.shape
    shard_len = parts[0].shape[1]
    me = lax.axis_index("seq")
    rows = heads * q_rows
    queries = q_ref[...].reshape(rows, HD)
    begin = jnp.concatenate([begin_ref[:, 0:1]] * heads, axis=0)
    place = lax.broadcasted_iota(jnp.int32, (rows, 1), 0) % q_rows
    qpos = (me + 1) * shard_len - q_rows + place
    scores = []
    for d, part in zip((0, 1, 3, 2), parts):
        count = part.shape[1]
        kpos = (me + 1 - d) * shard_len - count + lax.broadcasted_iota(jnp.int32, (1, count), 1)
        if count > shard_len:
            kpos = jnp.where(kpos < (me - d) * shard_len, kpos - shard_len, kpos)
        score = lax.dot_general(
            queries, part[0], (((1,), (1,)), ((), ())), preferred_element_type=F32
        )
        allowed = kpos >= begin
        if d == 0:
            allowed = allowed & (kpos <= qpos)
        scores.append(jnp.where(allowed, score, F32(-1e30)))
    peak = functools.reduce(jnp.maximum, [jnp.max(s, axis=1, keepdims=True) for s in scores])
    total = jnp.zeros((rows, 1), F32)
    acc = jnp.zeros((rows, HD), F32)
    for score, part in zip(scores, parts):
        weight = jnp.exp((score - peak) * F32(HD**-0.5))
        total = total + jnp.sum(weight, axis=1, keepdims=True)
        acc = acc + jnp.dot(weight.astype(BF16), part[1], preferred_element_type=F32)
    attended = (acc / total).astype(BF16)
    wide = jnp.concatenate([attended[h * q_rows : (h + 1) * q_rows] for h in range(heads)], axis=1)

    blocks, _, tokens = routes_ref.shape
    experts = out_ref.shape[0]
    slots = out_ref.shape[1]
    capacity = slots // blocks
    spread = lax.broadcasted_iota(jnp.int32, (tokens, q_rows), 0) == (
        lax.broadcasted_iota(jnp.int32, (tokens, q_rows), 1) % tokens
    )
    block_of = lax.broadcasted_iota(jnp.int32, (blocks, q_rows), 1) // tokens
    in_block = lax.broadcasted_iota(jnp.int32, (blocks, q_rows), 0) == block_of
    expert_id = lax.broadcasted_iota(jnp.int32, (experts, q_rows), 0).astype(F32)
    named = jnp.zeros((experts, q_rows), jnp.bool_)
    for k in range(2):
        chosen = routes_ref[:, k, :].astype(F32).astype(BF16)
        by_block = jnp.dot(chosen, spread.astype(BF16), preferred_element_type=F32)
        flat = jnp.sum(jnp.where(in_block, by_block, 0.0), axis=0, keepdims=True)
        named = named | (flat == expert_id)
    r = lax.broadcasted_iota(jnp.int32, (q_rows, q_rows), 0)
    c = lax.broadcasted_iota(jnp.int32, (q_rows, q_rows), 1)
    earlier = (r // tokens == c // tokens) & (r < c)
    ahead = jnp.dot(named.astype(BF16), earlier.astype(BF16), preferred_element_type=F32)
    token_block = lax.broadcasted_iota(jnp.int32, (experts, q_rows), 1) // tokens
    slot = jnp.where(named, ahead + (token_block * capacity).astype(F32), F32(-1))
    slot_id = lax.broadcasted_iota(jnp.int32, (slots, q_rows), 0).astype(F32)
    selector = jnp.concatenate(
        [(slot_id == slot[e : e + 1, :]).astype(F32) for e in range(experts)], axis=0
    ).astype(BF16)
    picked = jnp.dot(selector, wide, preferred_element_type=F32)
    out_ref[...] = picked.reshape(out_ref.shape).astype(BF16)


def pack(x_ref, out_ref):
    experts, _, chunk = x_ref.shape
    parts = [x_ref[e].astype(F32) for e in range(experts)]
    square = sum(jnp.sum(x * x, axis=1, keepdims=True) for x in parts)
    largest = functools.reduce(
        jnp.maximum, [jnp.max(jnp.abs(x), axis=1, keepdims=True) for x in parts]
    )
    largest = jnp.maximum(largest, F32(1e-30))
    up = F32(FIXED) / largest
    for e, x in enumerate(parts):
        fixed = jnp.round(x * up).astype(jnp.int32)
        out_ref[:, e * chunk : (e + 1) * chunk] = fixed.astype(jnp.int16)
    down = largest * F32(1 / FIXED) * lax.rsqrt(square / F32(experts * chunk) + F32(1e-05))
    power = jnp.floor(jnp.log2(down))
    digits = jnp.round(down * jnp.exp2(-power) * F32(DIGITS))
    tail = (x_ref.shape[1], out_ref.shape[1] - experts * chunk)
    lane = lax.broadcasted_iota(jnp.int32, tail, 1)
    factor = jnp.where(lane == 0, digits, jnp.where(lane == 1, power, F32(0)))
    out_ref[:, experts * chunk :] = factor.astype(jnp.int32).astype(jnp.int16)


def project(chunks, x_ref, w_ref, out_ref, w_vmem, sems):
    seq_count = x_ref.shape[0]
    depth = w_vmem.shape[0]
    chunk = depth // chunks

    def copy(e):
        at = pl.ds(e * chunk, chunk)
        return pltpu.make_async_copy(w_ref.at[0, at], w_vmem.at[at], sems.at[e])

    def rows(lo, size):
        part = [x_ref[s, :, lo : lo + size].astype(jnp.int32) for s in range(seq_count)]
        return jnp.concatenate(part, axis=0).astype(F32)

    for e in range(chunks):
        copy(e).start()
    factor = rows(depth, HD)
    factor = factor[:, 0:1] * F32(1 / DIGITS) * jnp.exp2(factor[:, 1:2])
    acc = jnp.zeros(out_ref.shape, F32)
    for e in range(chunks):
        x = rows(e * chunk, chunk).astype(BF16)
        copy(e).wait()
        acc = acc + jnp.dot(
            x, w_vmem[e * chunk : (e + 1) * chunk], preferred_element_type=F32
        )
    upper = acc * factor
    out_ref[...] = (upper / (1.0 + jnp.exp(-upper))).astype(BF16)


def mix(back_ref, selector_ref, column_ref, out_ref):
    units = back_ref.shape[2]
    for s in range(back_ref.shape[0]):
        both = F32(0)
        for k in range(2):
            rows = lax.dot_general(
                selector_ref[k],
                back_ref[s],
                (((0,), (0,)), ((), ())),
                preferred_element_type=F32,
            )
            both = both + rows * column_ref[k, :, 0:1]
        out_ref[:, s * units : (s + 1) * units] = both.astype(BF16)


def shards(queries, keys, values, lengths, routes, gates, w_up):
    q_rows, width = queries.shape
    shard_len = keys.shape[0]
    seq_count = lax.axis_size("seq")
    expert_count = lax.axis_size("expert")
    capacity = 3
    tok_count = routes.shape[0]
    per_expert = expert_count * capacity
    reach = LONGEST + shard_len
    reach = reach - (shard_len - q_rows)

    heads = width // HD
    keys, values, queries, lengths, routes, gates = (
        pltpu.with_memory_space_constraint(x, pltpu.HBM)
        for x in (keys, values, queries, lengths.reshape(1, -1), routes.T, gates.T)
    )
    hbm = pl.BlockSpec(memory_space=pltpu.HBM)
    kv_own, message = pl.pallas_call(
        first,
        out_shape=(
            jax.ShapeDtypeStruct((2, shard_len, HD), BF16),
            jax.ShapeDtypeStruct((expert_count, 2, tok_count), jnp.int32),
        ),
        in_specs=[hbm] * 3,
        out_specs=(VMEM,) * 2,
        scratch_shapes=[
            pltpu.VMEM(routes.shape, jnp.int32),
            pltpu.SemaphoreType.DMA((3,)),
        ],
        compiler_params=pltpu.CompilerParams(vmem_limit_bytes=8 << 20),
        name="first",
    )(keys, values, routes)
    q_heads, begin, selectors, columns = pl.pallas_call(
        functools.partial(second, shard_len),
        out_shape=(
            jax.ShapeDtypeStruct((heads, q_rows, HD), BF16),
            jax.ShapeDtypeStruct((q_rows, HD), jnp.int32),
            jax.ShapeDtypeStruct((2, per_expert, tok_count), BF16),
            jax.ShapeDtypeStruct((2, tok_count, HD), F32),
        ),
        in_specs=[hbm] * 4,
        out_specs=(VMEM,) * 4,
        scratch_shapes=[
            pltpu.VMEM(queries.shape, BF16),
            pltpu.VMEM(lengths.shape, jnp.int32),
            pltpu.VMEM(routes.shape, jnp.int32),
            pltpu.VMEM(gates.shape, F32),
            pltpu.SemaphoreType.DMA((4,)),
        ],
        compiler_params=pltpu.CompilerParams(vmem_limit_bytes=8 << 20),
        cost_estimate=pl.CostEstimate(flops=4_000_000, bytes_accessed=200_000, transcendentals=0),
        name="second",
    )(queries, lengths, routes, gates)
    by_one, by_three = ([(i, (i + d) % seq_count) for i in range(seq_count)] for d in (1, 3))
    far = lax.ppermute(kv_own, "seq", by_three)
    near = lax.ppermute(kv_own, "seq", by_one)
    beyond = pl.pallas_call(
        forward,
        out_shape=jax.ShapeDtypeStruct((2, reach - 3 * shard_len, HD), BF16),
        in_specs=[VMEM] * 2,
        out_specs=VMEM,
        compiler_params=pltpu.CompilerParams(vmem_limit_bytes=8 << 20),
        name="forward",
    )(near, far)
    beyond = lax.ppermute(beyond, "seq", by_one)
    parts = [kv_own, near, far, beyond]
    row_routes = exchange(message, "expert")

    outgoing = pl.pallas_call(
        attend,
        out_shape=jax.ShapeDtypeStruct((expert_count, per_expert, width), BF16),
        in_specs=[VMEM] * (3 + len(parts)),
        out_specs=VMEM,
        compiler_params=pltpu.CompilerParams(vmem_limit_bytes=24 << 20),
        name="attend",
    )(begin, row_routes, q_heads, *parts)
    landed = exchange(outgoing, "expert")
    packed = pl.pallas_call(
        pack,
        out_shape=jax.ShapeDtypeStruct((per_expert, expert_count * width + HD), jnp.int16),
        in_specs=[VMEM],
        out_specs=VMEM,
        compiler_params=pltpu.CompilerParams(vmem_limit_bytes=16 << 20),
        name="pack",
    )(landed)
    incoming = lax.all_gather(packed, "seq")
    act = pl.pallas_call(
        functools.partial(project, expert_count),
        out_shape=jax.ShapeDtypeStruct((seq_count * per_expert, w_up.shape[2]), BF16),
        in_specs=[VMEM, pl.BlockSpec(memory_space=pltpu.HBM)],
        out_specs=VMEM,
        scratch_shapes=[
            pltpu.VMEM(w_up.shape[1:], BF16),
            pltpu.SemaphoreType.DMA((expert_count,)),
        ],
        compiler_params=pltpu.CompilerParams(vmem_limit_bytes=32 << 20),
        name="project",
    )(incoming, pltpu.with_memory_space_constraint(w_up, pltpu.HBM))
    ff_local = act.shape[1]
    back = exchange(act.reshape(seq_count * expert_count, capacity, ff_local), ("seq", "expert"))
    back = back.reshape(seq_count, per_expert, ff_local)
    return pl.pallas_call(
        mix,
        out_shape=jax.ShapeDtypeStruct((tok_count, seq_count * ff_local), BF16),
        in_specs=[VMEM] * 3,
        out_specs=VMEM,
        compiler_params=pltpu.CompilerParams(vmem_limit_bytes=16 << 20),
        name="mix",
    )(back, selectors, columns)


def solution(mesh):
    placed = (
        P(("dp", "seq"), "expert"),
        P(("dp", "seq"), "expert"),
        P(("dp", "seq"), "expert"),
        P("dp"),
        P(("dp", "seq", "expert"), None),
        P(("dp", "seq", "expert"), None),
        P("expert", None, "seq"),
    )

    return jax.shard_map(
        shards,
        mesh=mesh,
        in_specs=placed,
        out_specs=P(("dp", "seq", "expert"), None),
        check_vma=False,
    )
```

```python
import functools

import jax
import jax.numpy as jnp
from jax import lax
from jax.experimental import pallas as pl
from jax.experimental.pallas import tpu as pltpu
from jax.sharding import PartitionSpec as P


HD = 128
LONGEST = 1024
FIXED = 32767
DIGITS = 8192
ROUTE_ROWS = 16
F32 = jnp.float32
BF16 = jnp.bfloat16
VMEM = pl.BlockSpec(memory_space=pltpu.VMEM)


def exchange(x, axis):
    return lax.all_to_all(x, axis, split_axis=0, concat_axis=0, tiled=True)


def worked_on():
    return lax.rem(lax.axis_index("seq") + 1, lax.axis_size("seq"))


def fetch(pairs, sems):
    copies = [pltpu.make_async_copy(a, b, sems.at[i]) for i, (a, b) in enumerate(pairs)]
    for copy in copies:
        copy.start()
    for copy in copies:
        copy.wait()


def first(keys_ref, values_ref, q_ref, routes_ref, kv_ref, left_ref, routes_vmem, sems):
    shard_len = keys_ref.shape[0]
    q_rows = q_ref.shape[0]
    heads = q_ref.shape[1] // HD
    pairs = [
        (keys_ref, kv_ref.at[0]),
        (values_ref, kv_ref.at[1]),
        (keys_ref, left_ref.at[pl.ds(0, shard_len)]),
        (values_ref, left_ref.at[pl.ds(shard_len, shard_len)]),
        (routes_ref, routes_vmem),
    ]
    for h in range(heads):
        pairs.append(
            (
                q_ref.at[:, pl.ds(h * HD, HD)],
                left_ref.at[pl.ds(2 * shard_len + h * q_rows, q_rows)],
            )
        )
    fetch(pairs, sems)
    at = 2 * shard_len + heads * q_rows
    size = left_ref.shape[0] - at
    choices, tokens = routes_vmem.shape
    left_ref[at:] = jnp.zeros((size, HD), BF16)
    left_ref[at : at + choices, :tokens] = routes_vmem[...].astype(F32).astype(BF16)


def forward(own_ref, near_ref, came_ref, out_ref, message_ref):
    rows = out_ref.shape[1] - own_ref.shape[1]
    out_ref[:, :rows] = near_ref[:, near_ref.shape[1] - rows :]
    out_ref[:, rows:] = own_ref[...]
    tail = came_ref[came_ref.shape[0] - ROUTE_ROWS :].astype(F32).astype(jnp.int32)
    _, choices, tokens = message_ref.shape
    message_ref[...] = jnp.broadcast_to(tail[:choices, :tokens][None], message_ref.shape)


def second(
    shard_len, q_rows,
    lengths_hbm, routes_hbm, gates_hbm,
    begin_ref, selector_ref, column_ref,
    lengths_ref, routes_ref, gates_ref, sems,
):
    pairs = [
        (lengths_hbm, lengths_ref),
        (routes_hbm, routes_ref),
        (gates_hbm, gates_ref),
    ]
    fetch(pairs, sems)
    routes = routes_ref[...]
    place = lax.broadcasted_iota(jnp.int32, begin_ref.shape, 0)
    qpos = (worked_on() + 1) * shard_len - q_rows + place
    begin = jnp.zeros(begin_ref.shape, jnp.int32)
    start = jnp.zeros((1, 1), jnp.int32)
    for j in range(lengths_ref.shape[1]):
        begin = jnp.where(start <= qpos, start, begin)
        start = start + lengths_ref[:, j : j + 1]
    begin_ref[...] = begin

    _, rows, tokens = selector_ref.shape
    capacity = 3
    row = lax.broadcasted_iota(jnp.int32, (rows, tokens), 0)
    named = [routes[k : k + 1, :] == row // capacity for k in range(2)]
    before = lax.broadcasted_iota(jnp.int32, (tokens, tokens), 0) < (
        lax.broadcasted_iota(jnp.int32, (tokens, tokens), 1)
    )
    either = (named[0] | named[1]).astype(F32).astype(BF16)
    ahead = jnp.dot(either, before.astype(F32).astype(BF16), preferred_element_type=F32)
    right = ahead == (row % capacity).astype(F32)
    diagonal = lax.broadcasted_iota(jnp.int32, (tokens, tokens), 0) == (
        lax.broadcasted_iota(jnp.int32, (tokens, tokens), 1)
    )
    for k in range(2):
        selector_ref[k] = (named[k] & right).astype(F32).astype(BF16)
        gate = jnp.where(diagonal, gates_ref[k : k + 1, :], F32(0))
        gate = jnp.sum(gate, axis=1, keepdims=True)
        column_ref[k] = jnp.broadcast_to(gate, column_ref.shape[1:])


def attend(begin_ref, routes_ref, came_ref, own_ref, near_ref, beyond_ref, out_ref):
    shard_len = own_ref.shape[1]
    q_rows = begin_ref.shape[0]
    heads = out_ref.shape[2] // HD
    me = worked_on()
    rows = heads * q_rows
    queries = came_ref[2 * shard_len : 2 * shard_len + rows]
    begin = jnp.concatenate([begin_ref[:, 0:1]] * heads, axis=0)
    place = lax.broadcasted_iota(jnp.int32, (rows, 1), 0) % q_rows
    qpos = (me + 1) * shard_len - q_rows + place
    parts = [(came_ref[:shard_len], came_ref[shard_len : 2 * shard_len])]
    parts += [(ref[0], ref[1]) for ref in (own_ref, near_ref, beyond_ref)]
    scores = []
    for d, (keys, _) in enumerate(parts):
        count = keys.shape[0]
        kpos = (me + 1 - d) * shard_len - count + lax.broadcasted_iota(jnp.int32, (1, count), 1)
        score = lax.dot_general(queries, keys, (((1,), (1,)), ((), ())), preferred_element_type=F32)
        allowed = kpos >= begin
        if d == 0:
            allowed = allowed & (kpos <= qpos)
        scores.append(jnp.where(allowed, score, F32(-1e30)))
    peak = functools.reduce(jnp.maximum, [jnp.max(s, axis=1, keepdims=True) for s in scores])
    total = jnp.zeros((rows, 1), F32)
    acc = jnp.zeros((rows, HD), F32)
    for score, (_, values) in zip(scores, parts):
        weight = jnp.exp((score - peak) * F32(HD**-0.5))
        total = total + jnp.sum(weight, axis=1, keepdims=True)
        acc = acc + jnp.dot(weight.astype(BF16), values, preferred_element_type=F32)
    attended = (acc / total).astype(BF16)
    wide = jnp.concatenate([attended[h * q_rows : (h + 1) * q_rows] for h in range(heads)], axis=1)

    blocks, _, tokens = routes_ref.shape
    experts = out_ref.shape[0]
    slots = out_ref.shape[1]
    capacity = slots // blocks
    spread = lax.broadcasted_iota(jnp.int32, (tokens, q_rows), 0) == (
        lax.broadcasted_iota(jnp.int32, (tokens, q_rows), 1) % tokens
    )
    block_of = lax.broadcasted_iota(jnp.int32, (blocks, q_rows), 1) // tokens
    in_block = lax.broadcasted_iota(jnp.int32, (blocks, q_rows), 0) == block_of
    expert_id = lax.broadcasted_iota(jnp.int32, (experts, q_rows), 0).astype(F32)
    named = jnp.zeros((experts, q_rows), jnp.bool_)
    for k in range(2):
        chosen = routes_ref[:, k, :].astype(F32).astype(BF16)
        by_block = jnp.dot(chosen, spread.astype(BF16), preferred_element_type=F32)
        flat = jnp.sum(jnp.where(in_block, by_block, 0.0), axis=0, keepdims=True)
        named = named | (flat == expert_id)
    r = lax.broadcasted_iota(jnp.int32, (q_rows, q_rows), 0)
    c = lax.broadcasted_iota(jnp.int32, (q_rows, q_rows), 1)
    earlier = (r // tokens == c // tokens) & (r < c)
    ahead = jnp.dot(named.astype(BF16), earlier.astype(BF16), preferred_element_type=F32)
    token_block = lax.broadcasted_iota(jnp.int32, (experts, q_rows), 1) // tokens
    slot = jnp.where(named, ahead + (token_block * capacity).astype(F32), F32(-1))
    slot_id = lax.broadcasted_iota(jnp.int32, (slots, q_rows), 0).astype(F32)
    selector = jnp.concatenate(
        [(slot_id == slot[e : e + 1, :]).astype(F32) for e in range(experts)], axis=0
    ).astype(BF16)
    picked = jnp.dot(selector, wide, preferred_element_type=F32)
    out_ref[...] = picked.reshape(out_ref.shape).astype(BF16)


def pack(x_ref, out_ref):
    experts, _, chunk = x_ref.shape
    parts = [x_ref[e].astype(F32) for e in range(experts)]
    square = sum(jnp.sum(x * x, axis=1, keepdims=True) for x in parts)
    largest = functools.reduce(
        jnp.maximum, [jnp.max(jnp.abs(x), axis=1, keepdims=True) for x in parts]
    )
    largest = jnp.maximum(largest, F32(1e-30))
    up = F32(FIXED) / largest
    for e, x in enumerate(parts):
        fixed = jnp.round(x * up).astype(jnp.int32)
        out_ref[:, e * chunk : (e + 1) * chunk] = fixed.astype(jnp.int16)
    down = largest * F32(1 / FIXED) * lax.rsqrt(square / F32(experts * chunk) + F32(1e-05))
    power = jnp.floor(jnp.log2(down))
    digits = jnp.round(down * jnp.exp2(-power) * F32(DIGITS))
    tail = (x_ref.shape[1], out_ref.shape[1] - experts * chunk)
    lane = lax.broadcasted_iota(jnp.int32, tail, 1)
    factor = jnp.where(lane == 0, digits, jnp.where(lane == 1, power, F32(0)))
    out_ref[:, experts * chunk :] = factor.astype(jnp.int32).astype(jnp.int16)


def project(chunks, x_ref, w_ref, out_ref, w_vmem, sems):
    seq_count = x_ref.shape[0]
    depth = w_vmem.shape[0]
    chunk = depth // chunks

    def copy(e):
        at = pl.ds(e * chunk, chunk)
        return pltpu.make_async_copy(w_ref.at[0, at], w_vmem.at[at], sems.at[e])

    def rows(lo, size):
        part = [x_ref[s - 1, :, lo : lo + size].astype(jnp.int32) for s in order]
        return jnp.concatenate(part, axis=0).astype(F32)

    order = [s or seq_count for s in range(seq_count)]

    for e in range(chunks):
        copy(e).start()
    factor = rows(depth, HD)
    factor = factor[:, 0:1] * F32(1 / DIGITS) * jnp.exp2(factor[:, 1:2])
    acc = jnp.zeros(out_ref.shape, F32)
    for e in range(chunks):
        x = rows(e * chunk, chunk).astype(BF16)
        copy(e).wait()
        acc = acc + jnp.dot(
            x, w_vmem[e * chunk : (e + 1) * chunk], preferred_element_type=F32
        )
    upper = acc * factor
    out_ref[...] = (upper / (1.0 + jnp.exp(-upper))).astype(BF16)


def mix(back_ref, selector_ref, column_ref, out_ref):
    units = back_ref.shape[2]
    for s in range(back_ref.shape[0]):
        both = F32(0)
        for k in range(2):
            rows = lax.dot_general(
                selector_ref[k],
                back_ref[s],
                (((0,), (0,)), ((), ())),
                preferred_element_type=F32,
            )
            both = both + rows * column_ref[k, :, 0:1]
        out_ref[:, s * units : (s + 1) * units] = both.astype(BF16)


def shards(queries, keys, values, lengths, routes, gates, w_up):
    q_rows, width = queries.shape
    shard_len = keys.shape[0]
    seq_count = lax.axis_size("seq")
    expert_count = lax.axis_size("expert")
    capacity = 3
    tok_count = routes.shape[0]
    per_expert = expert_count * capacity
    reach = LONGEST + shard_len
    reach = reach - (shard_len - q_rows)

    heads = width // HD
    keys, values, queries, lengths, routes, gates = (
        pltpu.with_memory_space_constraint(x, pltpu.HBM)
        for x in (keys, values, queries, lengths.reshape(1, -1), routes.T, gates.T)
    )
    hbm = pl.BlockSpec(memory_space=pltpu.HBM)
    small = pltpu.CompilerParams(vmem_limit_bytes=8 << 20)
    left_rows = 2 * shard_len + heads * q_rows + ROUTE_ROWS
    own, left = pl.pallas_call(
        first,
        out_shape=(
            jax.ShapeDtypeStruct((2, shard_len, HD), BF16),
            jax.ShapeDtypeStruct((left_rows, HD), BF16),
        ),
        in_specs=[hbm] * 4,
        out_specs=(VMEM,) * 2,
        scratch_shapes=[
            pltpu.VMEM(routes.shape, jnp.int32),
            pltpu.SemaphoreType.DMA((5 + heads,)),
        ],
        compiler_params=small,
        name="first",
    )(keys, values, queries, routes)
    begin, selectors, columns = pl.pallas_call(
        functools.partial(second, shard_len, q_rows),
        out_shape=(
            jax.ShapeDtypeStruct((q_rows, HD), jnp.int32),
            jax.ShapeDtypeStruct((2, per_expert, tok_count), BF16),
            jax.ShapeDtypeStruct((2, tok_count, HD), F32),
        ),
        in_specs=[hbm] * 3,
        out_specs=(VMEM,) * 3,
        scratch_shapes=[
            pltpu.VMEM(lengths.shape, jnp.int32),
            pltpu.VMEM(routes.shape, jnp.int32),
            pltpu.VMEM(gates.shape, F32),
            pltpu.SemaphoreType.DMA((3,)),
        ],
        compiler_params=small,
        cost_estimate=pl.CostEstimate(flops=4_000_000, bytes_accessed=200_000, transcendentals=0),
        name="second",
    )(lengths, routes, gates)

    def shifted(x, by):
        return lax.ppermute(x, "seq", [(i, (i + by) % seq_count) for i in range(seq_count)])

    came = shifted(left, -1)
    near = shifted(own, 1)
    beyond, message = pl.pallas_call(
        forward,
        out_shape=(
            jax.ShapeDtypeStruct((2, reach - 3 * shard_len, HD), BF16),
            jax.ShapeDtypeStruct((expert_count, 2, tok_count), jnp.int32),
        ),
        in_specs=[VMEM] * 3,
        out_specs=(VMEM,) * 2,
        compiler_params=small,
        name="forward",
    )(own, near, came)
    beyond = shifted(beyond, 2)
    row_routes = exchange(message, "expert")

    outgoing = pl.pallas_call(
        attend,
        out_shape=jax.ShapeDtypeStruct((expert_count, per_expert, width), BF16),
        in_specs=[VMEM] * 6,
        out_specs=VMEM,
        compiler_params=pltpu.CompilerParams(vmem_limit_bytes=24 << 20),
        name="attend",
    )(begin, row_routes, came, own, near, beyond)
    landed = exchange(outgoing, "expert")
    packed = pl.pallas_call(
        pack,
        out_shape=jax.ShapeDtypeStruct((per_expert, expert_count * width + HD), jnp.int16),
        in_specs=[VMEM],
        out_specs=VMEM,
        compiler_params=pltpu.CompilerParams(vmem_limit_bytes=16 << 20),
        name="pack",
    )(landed)
    incoming = lax.all_gather(packed, "seq")
    act = pl.pallas_call(
        functools.partial(project, expert_count),
        out_shape=jax.ShapeDtypeStruct((seq_count * per_expert, w_up.shape[2]), BF16),
        in_specs=[VMEM, pl.BlockSpec(memory_space=pltpu.HBM)],
        out_specs=VMEM,
        scratch_shapes=[
            pltpu.VMEM(w_up.shape[1:], BF16),
            pltpu.SemaphoreType.DMA((expert_count,)),
        ],
        compiler_params=pltpu.CompilerParams(vmem_limit_bytes=32 << 20),
        name="project",
    )(incoming, pltpu.with_memory_space_constraint(w_up, pltpu.HBM))
    ff_local = act.shape[1]
    back = exchange(act.reshape(seq_count * expert_count, capacity, ff_local), ("seq", "expert"))
    back = back.reshape(seq_count, per_expert, ff_local)
    return pl.pallas_call(
        mix,
        out_shape=jax.ShapeDtypeStruct((tok_count, seq_count * ff_local), BF16),
        in_specs=[VMEM] * 3,
        out_specs=VMEM,
        compiler_params=pltpu.CompilerParams(vmem_limit_bytes=16 << 20),
        name="mix",
    )(back, selectors, columns)


def solution(mesh):
    placed = (
        P(("dp", "seq"), "expert"),
        P(("dp", "seq"), "expert"),
        P(("dp", "seq"), "expert"),
        P("dp"),
        P(("dp", "seq", "expert"), None),
        P(("dp", "seq", "expert"), None),
        P("expert", None, "seq"),
    )

    return jax.shard_map(
        shards,
        mesh=mesh,
        in_specs=placed,
        out_specs=P(("dp", "seq", "expert"), None),
        check_vma=False,
    )
```

```python
import functools

import jax
import jax.numpy as jnp
from jax import lax
from jax.experimental import pallas as pl
from jax.experimental.pallas import tpu as pltpu
from jax.sharding import PartitionSpec as P


HD = 128
LONGEST = 1024
FIXED = 32767
DIGITS = 8192
F32 = jnp.float32
BF16 = jnp.bfloat16
VMEM = pl.BlockSpec(memory_space=pltpu.VMEM)


def exchange(x, axis):
    return lax.all_to_all(x, axis, split_axis=0, concat_axis=0, tiled=True)


def worked_on():
    return lax.rem(lax.axis_index("seq") + 1, lax.axis_size("seq"))


def fetch(pairs, sems):
    copies = [pltpu.make_async_copy(a, b, sems.at[i]) for i, (a, b) in enumerate(pairs)]
    for copy in copies:
        copy.start()
    for copy in copies:
        copy.wait()


def first(
    keys_ref, values_ref, q_ref, routes_ref,
    kv_ref, left_ref, message_ref,
    routes_vmem, sems,
):
    shard_len = keys_ref.shape[0]
    q_rows = q_ref.shape[0]
    heads = q_ref.shape[1] // HD
    pairs = [
        (keys_ref, kv_ref.at[0]),
        (values_ref, kv_ref.at[1]),
        (keys_ref, left_ref.at[pl.ds(0, shard_len)]),
        (values_ref, left_ref.at[pl.ds(shard_len, shard_len)]),
        (routes_ref, routes_vmem),
    ]
    for h in range(heads):
        pairs.append(
            (
                q_ref.at[:, pl.ds(h * HD, HD)],
                left_ref.at[pl.ds(2 * shard_len + h * q_rows, q_rows)],
            )
        )
    fetch(pairs, sems)
    message_ref[...] = jnp.broadcast_to(routes_vmem[...][None], message_ref.shape)


def forward(own_ref, near_ref, out_ref):
    rows = out_ref.shape[1] - own_ref.shape[1]
    out_ref[:, :rows] = near_ref[:, near_ref.shape[1] - rows :]
    out_ref[:, rows:] = own_ref[...]


def second(
    shard_len, q_rows,
    lengths_hbm, routes_hbm, gates_hbm,
    begin_ref, selector_ref, column_ref,
    lengths_ref, routes_ref, gates_ref, sems,
):
    pairs = [
        (lengths_hbm, lengths_ref),
        (routes_hbm, routes_ref),
        (gates_hbm, gates_ref),
    ]
    fetch(pairs, sems)
    routes = routes_ref[...]
    place = lax.broadcasted_iota(jnp.int32, begin_ref.shape, 0)
    qpos = (worked_on() + 1) * shard_len - q_rows + place
    begin = jnp.zeros(begin_ref.shape, jnp.int32)
    start = jnp.zeros((1, 1), jnp.int32)
    for j in range(lengths_ref.shape[1]):
        begin = jnp.where(start <= qpos, start, begin)
        start = start + lengths_ref[:, j : j + 1]
    begin_ref[...] = begin

    _, rows, tokens = selector_ref.shape
    capacity = 3
    row = lax.broadcasted_iota(jnp.int32, (rows, tokens), 0)
    named = [routes[k : k + 1, :] == row // capacity for k in range(2)]
    before = lax.broadcasted_iota(jnp.int32, (tokens, tokens), 0) < (
        lax.broadcasted_iota(jnp.int32, (tokens, tokens), 1)
    )
    either = (named[0] | named[1]).astype(F32).astype(BF16)
    ahead = jnp.dot(either, before.astype(F32).astype(BF16), preferred_element_type=F32)
    right = ahead == (row % capacity).astype(F32)
    diagonal = lax.broadcasted_iota(jnp.int32, (tokens, tokens), 0) == (
        lax.broadcasted_iota(jnp.int32, (tokens, tokens), 1)
    )
    for k in range(2):
        selector_ref[k] = (named[k] & right).astype(F32).astype(BF16)
        gate = jnp.where(diagonal, gates_ref[k : k + 1, :], F32(0))
        gate = jnp.sum(gate, axis=1, keepdims=True)
        column_ref[k] = jnp.broadcast_to(gate, column_ref.shape[1:])


def attend(begin_ref, routes_ref, came_ref, own_ref, near_ref, beyond_ref, out_ref):
    shard_len = own_ref.shape[1]
    q_rows = begin_ref.shape[0]
    heads = out_ref.shape[2] // HD
    me = worked_on()
    rows = heads * q_rows
    queries = came_ref[2 * shard_len : 2 * shard_len + rows]
    begin = jnp.concatenate([begin_ref[:, 0:1]] * heads, axis=0)
    place = lax.broadcasted_iota(jnp.int32, (rows, 1), 0) % q_rows
    qpos = (me + 1) * shard_len - q_rows + place
    parts = [(came_ref[:shard_len], came_ref[shard_len : 2 * shard_len])]
    parts += [(ref[0], ref[1]) for ref in (own_ref, near_ref, beyond_ref)]
    scores = []
    for d, (keys, _) in enumerate(parts):
        count = keys.shape[0]
        kpos = (me + 1 - d) * shard_len - count + lax.broadcasted_iota(jnp.int32, (1, count), 1)
        score = lax.dot_general(queries, keys, (((1,), (1,)), ((), ())), preferred_element_type=F32)
        allowed = kpos >= begin
        if d == 0:
            allowed = allowed & (kpos <= qpos)
        scores.append(jnp.where(allowed, score, F32(-1e30)))
    peak = functools.reduce(jnp.maximum, [jnp.max(s, axis=1, keepdims=True) for s in scores])
    total = jnp.zeros((rows, 1), F32)
    acc = jnp.zeros((rows, HD), F32)
    for score, (_, values) in zip(scores, parts):
        weight = jnp.exp((score - peak) * F32(HD**-0.5))
        total = total + jnp.sum(weight, axis=1, keepdims=True)
        acc = acc + jnp.dot(weight.astype(BF16), values, preferred_element_type=F32)
    attended = (acc / total).astype(BF16)
    wide = jnp.concatenate([attended[h * q_rows : (h + 1) * q_rows] for h in range(heads)], axis=1)

    experts = out_ref.shape[0]
    blocks = routes_ref.shape[0] // lax.axis_size("seq")
    tokens = routes_ref.shape[2]
    mine = routes_ref[pl.ds(me * blocks, blocks)].astype(F32)
    slots = out_ref.shape[1]
    capacity = slots // blocks
    spread = lax.broadcasted_iota(jnp.int32, (tokens, q_rows), 0) == (
        lax.broadcasted_iota(jnp.int32, (tokens, q_rows), 1) % tokens
    )
    block_of = lax.broadcasted_iota(jnp.int32, (blocks, q_rows), 1) // tokens
    in_block = lax.broadcasted_iota(jnp.int32, (blocks, q_rows), 0) == block_of
    expert_id = lax.broadcasted_iota(jnp.int32, (experts, q_rows), 0).astype(F32)
    named = jnp.zeros((experts, q_rows), jnp.bool_)
    for k in range(2):
        chosen = mine[:, k, :].astype(BF16)
        by_block = jnp.dot(chosen, spread.astype(BF16), preferred_element_type=F32)
        flat = jnp.sum(jnp.where(in_block, by_block, 0.0), axis=0, keepdims=True)
        named = named | (flat == expert_id)
    r = lax.broadcasted_iota(jnp.int32, (q_rows, q_rows), 0)
    c = lax.broadcasted_iota(jnp.int32, (q_rows, q_rows), 1)
    earlier = (r // tokens == c // tokens) & (r < c)
    ahead = jnp.dot(named.astype(BF16), earlier.astype(BF16), preferred_element_type=F32)
    token_block = lax.broadcasted_iota(jnp.int32, (experts, q_rows), 1) // tokens
    slot = jnp.where(named, ahead + (token_block * capacity).astype(F32), F32(-1))
    slot_id = lax.broadcasted_iota(jnp.int32, (slots, q_rows), 0).astype(F32)
    selector = jnp.concatenate(
        [(slot_id == slot[e : e + 1, :]).astype(F32) for e in range(experts)], axis=0
    ).astype(BF16)
    picked = jnp.dot(selector, wide, preferred_element_type=F32)
    out_ref[...] = picked.reshape(out_ref.shape).astype(BF16)


def pack(x_ref, out_ref):
    experts, _, chunk = x_ref.shape
    parts = [x_ref[e].astype(F32) for e in range(experts)]
    square = sum(jnp.sum(x * x, axis=1, keepdims=True) for x in parts)
    largest = functools.reduce(
        jnp.maximum, [jnp.max(jnp.abs(x), axis=1, keepdims=True) for x in parts]
    )
    largest = jnp.maximum(largest, F32(1e-30))
    up = F32(FIXED) / largest
    for e, x in enumerate(parts):
        fixed = jnp.round(x * up).astype(jnp.int32)
        out_ref[:, e * chunk : (e + 1) * chunk] = fixed.astype(jnp.int16)
    down = largest * F32(1 / FIXED) * lax.rsqrt(square / F32(experts * chunk) + F32(1e-05))
    power = jnp.floor(jnp.log2(down))
    digits = jnp.round(down * jnp.exp2(-power) * F32(DIGITS))
    tail = (x_ref.shape[1], out_ref.shape[1] - experts * chunk)
    lane = lax.broadcasted_iota(jnp.int32, tail, 1)
    factor = jnp.where(lane == 0, digits, jnp.where(lane == 1, power, F32(0)))
    out_ref[:, experts * chunk :] = factor.astype(jnp.int32).astype(jnp.int16)


def project(chunks, x_ref, w_ref, out_ref, w_vmem, sems):
    seq_count = x_ref.shape[0]
    depth = w_vmem.shape[0]
    chunk = depth // chunks

    def copy(e):
        at = pl.ds(e * chunk, chunk)
        return pltpu.make_async_copy(w_ref.at[0, at], w_vmem.at[at], sems.at[e])

    def rows(lo, size):
        part = [x_ref[s - 1, :, lo : lo + size].astype(jnp.int32) for s in order]
        return jnp.concatenate(part, axis=0).astype(F32)

    order = [s or seq_count for s in range(seq_count)]

    for e in range(chunks):
        copy(e).start()
    factor = rows(depth, HD)
    factor = factor[:, 0:1] * F32(1 / DIGITS) * jnp.exp2(factor[:, 1:2])
    acc = jnp.zeros(out_ref.shape, F32)
    for e in range(chunks):
        x = rows(e * chunk, chunk).astype(BF16)
        copy(e).wait()
        acc = acc + jnp.dot(
            x, w_vmem[e * chunk : (e + 1) * chunk], preferred_element_type=F32
        )
    upper = acc * factor
    out_ref[...] = (upper / (1.0 + jnp.exp(-upper))).astype(BF16)


def mix(back_ref, selector_ref, column_ref, out_ref):
    units = back_ref.shape[2]
    for s in range(back_ref.shape[0]):
        both = F32(0)
        for k in range(2):
            rows = lax.dot_general(
                selector_ref[k],
                back_ref[s],
                (((0,), (0,)), ((), ())),
                preferred_element_type=F32,
            )
            both = both + rows * column_ref[k, :, 0:1]
        out_ref[:, s * units : (s + 1) * units] = both.astype(BF16)


def shards(queries, keys, values, lengths, routes, gates, w_up):
    q_rows, width = queries.shape
    shard_len = keys.shape[0]
    seq_count = lax.axis_size("seq")
    expert_count = lax.axis_size("expert")
    capacity = 3
    tok_count = routes.shape[0]
    per_expert = expert_count * capacity
    reach = LONGEST + shard_len
    reach = reach - (shard_len - q_rows)

    heads = width // HD
    keys, values, queries, lengths, routes, gates = (
        pltpu.with_memory_space_constraint(x, pltpu.HBM)
        for x in (keys, values, queries, lengths.reshape(1, -1), routes.T, gates.T)
    )
    hbm = pl.BlockSpec(memory_space=pltpu.HBM)
    small = pltpu.CompilerParams(vmem_limit_bytes=8 << 20)
    left_rows = 2 * shard_len + heads * q_rows
    own, left, message = pl.pallas_call(
        first,
        out_shape=(
            jax.ShapeDtypeStruct((2, shard_len, HD), BF16),
            jax.ShapeDtypeStruct((left_rows, HD), BF16),
            jax.ShapeDtypeStruct((seq_count * expert_count, 2, tok_count), jnp.int32),
        ),
        in_specs=[hbm] * 4,
        out_specs=(VMEM,) * 3,
        scratch_shapes=[
            pltpu.VMEM(routes.shape, jnp.int32),
            pltpu.SemaphoreType.DMA((5 + heads,)),
        ],
        compiler_params=small,
        name="first",
    )(keys, values, queries, routes)
    begin, selectors, columns = pl.pallas_call(
        functools.partial(second, shard_len, q_rows),
        out_shape=(
            jax.ShapeDtypeStruct((q_rows, HD), jnp.int32),
            jax.ShapeDtypeStruct((2, per_expert, tok_count), BF16),
            jax.ShapeDtypeStruct((2, tok_count, HD), F32),
        ),
        in_specs=[hbm] * 3,
        out_specs=(VMEM,) * 3,
        scratch_shapes=[
            pltpu.VMEM(lengths.shape, jnp.int32),
            pltpu.VMEM(routes.shape, jnp.int32),
            pltpu.VMEM(gates.shape, F32),
            pltpu.SemaphoreType.DMA((3,)),
        ],
        compiler_params=small,
        cost_estimate=pl.CostEstimate(flops=4_000_000, bytes_accessed=200_000, transcendentals=0),
        name="second",
    )(lengths, routes, gates)

    def shifted(x, by):
        return lax.ppermute(x, "seq", [(i, (i + by) % seq_count) for i in range(seq_count)])

    came = shifted(left, -1)
    near = shifted(own, 1)
    all_routes = exchange(message, ("seq", "expert"))
    beyond = pl.pallas_call(
        forward,
        out_shape=jax.ShapeDtypeStruct((2, reach - 3 * shard_len, HD), BF16),
        in_specs=[VMEM] * 2,
        out_specs=VMEM,
        compiler_params=small,
        name="forward",
    )(own, near)
    beyond = shifted(beyond, 2)

    outgoing = pl.pallas_call(
        attend,
        out_shape=jax.ShapeDtypeStruct((expert_count, per_expert, width), BF16),
        in_specs=[VMEM] * 6,
        out_specs=VMEM,
        compiler_params=pltpu.CompilerParams(vmem_limit_bytes=24 << 20),
        name="attend",
    )(begin, all_routes, came, own, near, beyond)
    landed = exchange(outgoing, "expert")
    packed = pl.pallas_call(
        pack,
        out_shape=jax.ShapeDtypeStruct((per_expert, expert_count * width + HD), jnp.int16),
        in_specs=[VMEM],
        out_specs=VMEM,
        compiler_params=pltpu.CompilerParams(vmem_limit_bytes=16 << 20),
        name="pack",
    )(landed)
    incoming = lax.all_gather(packed, "seq")
    act = pl.pallas_call(
        functools.partial(project, expert_count),
        out_shape=jax.ShapeDtypeStruct((seq_count * per_expert, w_up.shape[2]), BF16),
        in_specs=[VMEM, pl.BlockSpec(memory_space=pltpu.HBM)],
        out_specs=VMEM,
        scratch_shapes=[
            pltpu.VMEM(w_up.shape[1:], BF16),
            pltpu.SemaphoreType.DMA((expert_count,)),
        ],
        compiler_params=pltpu.CompilerParams(vmem_limit_bytes=32 << 20),
        name="project",
    )(incoming, pltpu.with_memory_space_constraint(w_up, pltpu.HBM))
    ff_local = act.shape[1]
    back = exchange(act.reshape(seq_count * expert_count, capacity, ff_local), ("seq", "expert"))
    back = back.reshape(seq_count, per_expert, ff_local)
    return pl.pallas_call(
        mix,
        out_shape=jax.ShapeDtypeStruct((tok_count, seq_count * ff_local), BF16),
        in_specs=[VMEM] * 3,
        out_specs=VMEM,
        compiler_params=pltpu.CompilerParams(vmem_limit_bytes=16 << 20),
        name="mix",
    )(back, selectors, columns)


def solution(mesh):
    placed = (
        P(("dp", "seq"), "expert"),
        P(("dp", "seq"), "expert"),
        P(("dp", "seq"), "expert"),
        P("dp"),
        P(("dp", "seq", "expert"), None),
        P(("dp", "seq", "expert"), None),
        P("expert", None, "seq"),
    )

    return jax.shard_map(
        shards,
        mesh=mesh,
        in_specs=placed,
        out_specs=P(("dp", "seq", "expert"), None),
        check_vma=False,
    )
```

```python
import functools

import jax
import jax.numpy as jnp
from jax import lax
from jax.experimental import pallas as pl
from jax.experimental.pallas import tpu as pltpu
from jax.sharding import PartitionSpec as P


HD = 128
LONGEST = 1024
FIXED = 32767
DIGITS = 8192
PEERS = 8
ROUTE_ROWS = 16
F32 = jnp.float32
BF16 = jnp.bfloat16
VMEM = pl.BlockSpec(memory_space=pltpu.VMEM)


def exchange(x, axis):
    return lax.all_to_all(x, axis, split_axis=0, concat_axis=0, tiled=True)


def worked_on():
    return lax.rem(lax.axis_index("seq") + 1, lax.axis_size("seq"))


def fetch(pairs, sems):
    copies = [pltpu.make_async_copy(a, b, sems.at[i]) for i, (a, b) in enumerate(pairs)]
    for copy in copies:
        copy.start()
    for copy in copies:
        copy.wait()


def first(keys_ref, values_ref, q_ref, routes_ref, kv_ref, left_ref, routes_vmem, sems):
    shard_len = keys_ref.shape[0]
    q_rows = q_ref.shape[0]
    heads = q_ref.shape[1] // HD
    pairs = [
        (keys_ref, kv_ref.at[0]),
        (values_ref, kv_ref.at[1]),
        (keys_ref, left_ref.at[pl.ds(0, shard_len)]),
        (values_ref, left_ref.at[pl.ds(shard_len, shard_len)]),
        (routes_ref, routes_vmem),
    ]
    for h in range(heads):
        pairs.append(
            (
                q_ref.at[:, pl.ds(h * HD, HD)],
                left_ref.at[pl.ds(2 * shard_len + h * q_rows, q_rows)],
            )
        )
    fetch(pairs, sems)
    at = 2 * shard_len + heads * q_rows
    size = left_ref.shape[0] - at
    choices, tokens = routes_vmem.shape
    left_ref[at:] = jnp.zeros((size, HD), BF16)
    left_ref[at : at + choices, :tokens] = routes_vmem[...].astype(F32).astype(BF16)


def forward(own_ref, near_ref, came_ref, out_ref, message_ref):
    rows = out_ref.shape[1] - own_ref.shape[1]
    out_ref[:, :rows] = near_ref[:, near_ref.shape[1] - rows :]
    out_ref[:, rows:] = own_ref[...]
    tail = came_ref[came_ref.shape[0] - ROUTE_ROWS :].astype(F32).astype(jnp.int32)
    _, choices, tokens = message_ref.shape
    message_ref[...] = jnp.broadcast_to(tail[:choices, :tokens][None], message_ref.shape)


def second(
    shard_len, q_rows,
    lengths_hbm, routes_hbm, gates_hbm,
    begin_ref, selector_ref, column_ref,
    lengths_ref, routes_ref, gates_ref, sems,
):
    pairs = [
        (lengths_hbm, lengths_ref),
        (routes_hbm, routes_ref),
        (gates_hbm, gates_ref),
    ]
    fetch(pairs, sems)
    routes = routes_ref[...]
    place = lax.broadcasted_iota(jnp.int32, begin_ref.shape, 0)
    qpos = (worked_on() + 1) * shard_len - q_rows + place
    begin = jnp.zeros(begin_ref.shape, jnp.int32)
    start = jnp.zeros((1, 1), jnp.int32)
    for j in range(lengths_ref.shape[1]):
        begin = jnp.where(start <= qpos, start, begin)
        start = start + lengths_ref[:, j : j + 1]
    begin_ref[...] = begin

    _, rows, tokens = selector_ref.shape
    capacity = 3
    row = lax.broadcasted_iota(jnp.int32, (rows, tokens), 0)
    named = [routes[k : k + 1, :] == row // capacity for k in range(2)]
    before = lax.broadcasted_iota(jnp.int32, (tokens, tokens), 0) < (
        lax.broadcasted_iota(jnp.int32, (tokens, tokens), 1)
    )
    either = (named[0] | named[1]).astype(F32).astype(BF16)
    ahead = jnp.dot(either, before.astype(F32).astype(BF16), preferred_element_type=F32)
    right = ahead == (row % capacity).astype(F32)
    diagonal = lax.broadcasted_iota(jnp.int32, (tokens, tokens), 0) == (
        lax.broadcasted_iota(jnp.int32, (tokens, tokens), 1)
    )
    for k in range(2):
        selector_ref[k] = (named[k] & right).astype(F32).astype(BF16)
        gate = jnp.where(diagonal, gates_ref[k : k + 1, :], F32(0))
        gate = jnp.sum(gate, axis=1, keepdims=True)
        column_ref[k] = jnp.broadcast_to(gate, column_ref.shape[1:])


def attend(begin_ref, routes_ref, came_ref, own_ref, near_ref, beyond_ref, out_ref):
    shard_len = own_ref.shape[1]
    q_rows = begin_ref.shape[0]
    heads = out_ref.shape[2] // HD
    me = worked_on()
    rows = heads * q_rows
    queries = came_ref[2 * shard_len : 2 * shard_len + rows]
    begin = jnp.concatenate([begin_ref[:, 0:1]] * heads, axis=0)
    place = lax.broadcasted_iota(jnp.int32, (rows, 1), 0) % q_rows
    qpos = (me + 1) * shard_len - q_rows + place
    parts = [(came_ref[:shard_len], came_ref[shard_len : 2 * shard_len])]
    parts += [(ref[0], ref[1]) for ref in (own_ref, near_ref, beyond_ref)]
    scores = []
    for d, (keys, _) in enumerate(parts):
        count = keys.shape[0]
        kpos = (me + 1 - d) * shard_len - count + lax.broadcasted_iota(jnp.int32, (1, count), 1)
        score = lax.dot_general(queries, keys, (((1,), (1,)), ((), ())), preferred_element_type=F32)
        allowed = kpos >= begin
        if d == 0:
            allowed = allowed & (kpos <= qpos)
        scores.append(jnp.where(allowed, score, F32(-1e30)))
    peak = functools.reduce(jnp.maximum, [jnp.max(s, axis=1, keepdims=True) for s in scores])
    total = jnp.zeros((rows, 1), F32)
    acc = jnp.zeros((rows, HD), F32)
    for score, (_, values) in zip(scores, parts):
        weight = jnp.exp((score - peak) * F32(HD**-0.5))
        total = total + jnp.sum(weight, axis=1, keepdims=True)
        acc = acc + jnp.dot(weight.astype(BF16), values, preferred_element_type=F32)
    attended = (acc / total).astype(BF16)
    wide = jnp.concatenate([attended[h * q_rows : (h + 1) * q_rows] for h in range(heads)], axis=1)

    blocks, _, tokens = routes_ref.shape
    experts = out_ref.shape[0]
    slots = out_ref.shape[1]
    spread = lax.broadcasted_iota(jnp.int32, (tokens, q_rows), 0) == (
        lax.broadcasted_iota(jnp.int32, (tokens, q_rows), 1) % tokens
    )
    block_of = lax.broadcasted_iota(jnp.int32, (blocks, q_rows), 1) // tokens
    in_block = lax.broadcasted_iota(jnp.int32, (blocks, q_rows), 0) == block_of
    expert_id = lax.broadcasted_iota(jnp.int32, (experts, q_rows), 0).astype(F32)
    named = jnp.zeros((experts, q_rows), jnp.bool_)
    for k in range(2):
        chosen = routes_ref[:, k, :].astype(F32).astype(BF16)
        by_block = jnp.dot(chosen, spread.astype(BF16), preferred_element_type=F32)
        flat = jnp.sum(jnp.where(in_block, by_block, 0.0), axis=0, keepdims=True)
        named = named | (flat == expert_id)
    r = lax.broadcasted_iota(jnp.int32, (q_rows, q_rows), 0)
    c = lax.broadcasted_iota(jnp.int32, (q_rows, q_rows), 1)
    earlier = (r // tokens == c // tokens) & (r < c)
    ahead = jnp.dot(named.astype(BF16), earlier.astype(BF16), preferred_element_type=F32)
    token_block = lax.broadcasted_iota(jnp.int32, (experts, q_rows), 1) // tokens
    slot = jnp.where(named, ahead * F32(blocks) + token_block.astype(F32), F32(-1))
    slot_id = lax.broadcasted_iota(jnp.int32, (slots, q_rows), 0).astype(F32)
    selector = jnp.concatenate(
        [(slot_id == slot[e : e + 1, :]).astype(F32) for e in range(experts)], axis=0
    ).astype(BF16)
    picked = jnp.dot(selector, wide, preferred_element_type=F32)
    out_ref[...] = picked.reshape(out_ref.shape).astype(BF16)


def pack(x_ref, out_ref):
    experts, _, chunk = x_ref.shape
    parts = [x_ref[e].astype(F32) for e in range(experts)]
    square = sum(jnp.sum(x * x, axis=1, keepdims=True) for x in parts)
    largest = functools.reduce(
        jnp.maximum, [jnp.max(jnp.abs(x), axis=1, keepdims=True) for x in parts]
    )
    largest = jnp.maximum(largest, F32(1e-30))
    up = F32(FIXED) / largest
    for e, x in enumerate(parts):
        fixed = jnp.round(x * up).astype(jnp.int32)
        out_ref[:, e * chunk : (e + 1) * chunk] = fixed.astype(jnp.int16)
    down = largest * F32(1 / FIXED) * lax.rsqrt(square / F32(experts * chunk) + F32(1e-05))
    power = jnp.floor(jnp.log2(down))
    digits = jnp.round(down * jnp.exp2(-power) * F32(DIGITS))
    tail = (x_ref.shape[1], out_ref.shape[1] - experts * chunk)
    lane = lax.broadcasted_iota(jnp.int32, tail, 1)
    factor = jnp.where(lane == 0, digits, jnp.where(lane == 1, power, F32(0)))
    out_ref[:, experts * chunk :] = factor.astype(jnp.int32).astype(jnp.int16)


def project(chunks, x_ref, w_ref, out_ref, w_vmem, sems):
    seq_count = x_ref.shape[0]
    depth = w_vmem.shape[0]
    chunk = depth // chunks

    def copy(e):
        at = pl.ds(e * chunk, chunk)
        return pltpu.make_async_copy(w_ref.at[0, at], w_vmem.at[at], sems.at[e])

    def rows(lo, size):
        part = [x_ref[s - 1, :, lo : lo + size].astype(jnp.int32) for s in order]
        return jnp.concatenate(part, axis=0).astype(F32)

    order = [s or seq_count for s in range(seq_count)]

    for e in range(chunks):
        copy(e).start()
    factor = rows(depth, HD)
    factor = factor[:, 0:1] * F32(1 / DIGITS) * jnp.exp2(factor[:, 1:2])
    acc = jnp.zeros((seq_count * x_ref.shape[1], w_vmem.shape[1]), F32)
    for e in range(chunks):
        x = rows(e * chunk, chunk).astype(BF16)
        copy(e).wait()
        acc = acc + jnp.dot(
            x, w_vmem[e * chunk : (e + 1) * chunk], preferred_element_type=F32
        )
    upper = acc * factor
    act = (upper / (1.0 + jnp.exp(-upper))).reshape(-1, PEERS, upper.shape[1])
    tiles = upper.shape[1] // HD
    parts = [act[:, :, j * HD : (j + 1) * HD] for j in range(tiles)]
    parts += [jnp.zeros_like(parts[0])] * (PEERS - tiles)
    turned = jnp.swapaxes(jnp.stack(parts, axis=1), 1, 2).astype(BF16)
    slots = out_ref.shape[1] // PEERS
    for s in range(seq_count):
        for c in range(slots):
            at = pl.ds(c * PEERS, PEERS)
            out_ref[s * PEERS : (s + 1) * PEERS, at] = turned[s * slots + c]


def mix(back_ref, selector_ref, column_ref, out_ref):
    seq_count = back_ref.shape[0] // PEERS
    units = out_ref.shape[1] // seq_count
    tiles = units // HD
    rows = selector_ref.shape[1]
    for s in range(seq_count):
        back = back_ref[s * PEERS : (s + 1) * PEERS].astype(F32)
        back = jnp.swapaxes(back.reshape(rows // PEERS, PEERS, PEERS, HD), 1, 2)
        wide = [back[:, j].reshape(rows, HD) for j in range(tiles)]
        wide = jnp.concatenate(wide, axis=1).astype(BF16)
        both = F32(0)
        for k in range(2):
            picked = lax.dot_general(
                selector_ref[k], wide, (((0,), (0,)), ((), ())), preferred_element_type=F32
            )
            both = both + picked * column_ref[k, :, 0:1]
        out_ref[:, s * units : (s + 1) * units] = both.astype(BF16)


def shards(queries, keys, values, lengths, routes, gates, w_up):
    q_rows, width = queries.shape
    shard_len = keys.shape[0]
    seq_count = lax.axis_size("seq")
    expert_count = lax.axis_size("expert")
    capacity = 3
    tok_count = routes.shape[0]
    per_expert = expert_count * capacity
    reach = LONGEST + shard_len
    reach = reach - (shard_len - q_rows)

    heads = width // HD
    keys, values, queries, lengths, routes, gates = (
        pltpu.with_memory_space_constraint(x, pltpu.HBM)
        for x in (keys, values, queries, lengths.reshape(1, -1), routes.T, gates.T)
    )
    hbm = pl.BlockSpec(memory_space=pltpu.HBM)
    small = pltpu.CompilerParams(vmem_limit_bytes=8 << 20)
    left_rows = 2 * shard_len + heads * q_rows + ROUTE_ROWS
    own, left = pl.pallas_call(
        first,
        out_shape=(
            jax.ShapeDtypeStruct((2, shard_len, HD), BF16),
            jax.ShapeDtypeStruct((left_rows, HD), BF16),
        ),
        in_specs=[hbm] * 4,
        out_specs=(VMEM,) * 2,
        scratch_shapes=[
            pltpu.VMEM(routes.shape, jnp.int32),
            pltpu.SemaphoreType.DMA((5 + heads,)),
        ],
        compiler_params=small,
        name="first",
    )(keys, values, queries, routes)
    begin, selectors, columns = pl.pallas_call(
        functools.partial(second, shard_len, q_rows),
        out_shape=(
            jax.ShapeDtypeStruct((q_rows, HD), jnp.int32),
            jax.ShapeDtypeStruct((2, per_expert, tok_count), BF16),
            jax.ShapeDtypeStruct((2, tok_count, HD), F32),
        ),
        in_specs=[hbm] * 3,
        out_specs=(VMEM,) * 3,
        scratch_shapes=[
            pltpu.VMEM(lengths.shape, jnp.int32),
            pltpu.VMEM(routes.shape, jnp.int32),
            pltpu.VMEM(gates.shape, F32),
            pltpu.SemaphoreType.DMA((3,)),
        ],
        compiler_params=small,
        cost_estimate=pl.CostEstimate(flops=4_000_000, bytes_accessed=200_000, transcendentals=0),
        name="second",
    )(lengths, routes, gates)

    def shifted(x, by):
        return lax.ppermute(x, "seq", [(i, (i + by) % seq_count) for i in range(seq_count)])

    came = shifted(left, -1)
    near = shifted(own, 1)
    beyond, message = pl.pallas_call(
        forward,
        out_shape=(
            jax.ShapeDtypeStruct((2, reach - 3 * shard_len, HD), BF16),
            jax.ShapeDtypeStruct((expert_count, 2, tok_count), jnp.int32),
        ),
        in_specs=[VMEM] * 3,
        out_specs=(VMEM,) * 2,
        compiler_params=small,
        name="forward",
    )(own, near, came)
    beyond = shifted(beyond, 2)
    row_routes = exchange(message, "expert")

    outgoing = pl.pallas_call(
        attend,
        out_shape=jax.ShapeDtypeStruct((expert_count, per_expert, width), BF16),
        in_specs=[VMEM] * 6,
        out_specs=VMEM,
        compiler_params=pltpu.CompilerParams(vmem_limit_bytes=24 << 20),
        name="attend",
    )(begin, row_routes, came, own, near, beyond)
    landed = exchange(outgoing, "expert")
    packed = pl.pallas_call(
        pack,
        out_shape=jax.ShapeDtypeStruct((per_expert, expert_count * width + HD), jnp.int16),
        in_specs=[VMEM],
        out_specs=VMEM,
        compiler_params=pltpu.CompilerParams(vmem_limit_bytes=16 << 20),
        name="pack",
    )(landed)
    incoming = lax.all_gather(packed, "seq")
    act = pl.pallas_call(
        functools.partial(project, expert_count),
        out_shape=jax.ShapeDtypeStruct((seq_count * expert_count, per_expert, HD), BF16),
        in_specs=[VMEM, pl.BlockSpec(memory_space=pltpu.HBM)],
        out_specs=VMEM,
        scratch_shapes=[
            pltpu.VMEM(w_up.shape[1:], BF16),
            pltpu.SemaphoreType.DMA((expert_count,)),
        ],
        compiler_params=pltpu.CompilerParams(vmem_limit_bytes=32 << 20),
        name="project",
    )(incoming, pltpu.with_memory_space_constraint(w_up, pltpu.HBM))
    back = exchange(act, ("seq", "expert"))
    return pl.pallas_call(
        mix,
        out_shape=jax.ShapeDtypeStruct((tok_count, seq_count * w_up.shape[2]), BF16),
        in_specs=[VMEM] * 3,
        out_specs=VMEM,
        compiler_params=pltpu.CompilerParams(vmem_limit_bytes=16 << 20),
        name="mix",
    )(back, selectors, columns)


def solution(mesh):
    placed = (
        P(("dp", "seq"), "expert"),
        P(("dp", "seq"), "expert"),
        P(("dp", "seq"), "expert"),
        P("dp"),
        P(("dp", "seq", "expert"), None),
        P(("dp", "seq", "expert"), None),
        P("expert", None, "seq"),
    )

    return jax.shard_map(
        shards,
        mesh=mesh,
        in_specs=placed,
        out_specs=P(("dp", "seq", "expert"), None),
        check_vma=False,
    )
```

```python
import functools

import jax
import jax.numpy as jnp
from jax import lax
from jax.experimental import pallas as pl
from jax.experimental.pallas import tpu as pltpu
from jax.sharding import PartitionSpec as P


HD = 128
LONGEST = 1024
FIXED = 32767
DIGITS = 8192
PEERS = 8
ROUTE_ROWS = 16
F32 = jnp.float32
BF16 = jnp.bfloat16
VMEM = pl.BlockSpec(memory_space=pltpu.VMEM)


def exchange(x, axis):
    return lax.all_to_all(x, axis, split_axis=0, concat_axis=0, tiled=True)


def worked_on():
    return lax.rem(lax.axis_index("seq") + 1, lax.axis_size("seq"))


def fetch(pairs, sems):
    copies = [pltpu.make_async_copy(a, b, sems.at[i]) for i, (a, b) in enumerate(pairs)]
    for copy in copies:
        copy.start()
    for copy in copies:
        copy.wait()


def first(keys_ref, values_ref, q_ref, routes_ref, kv_ref, left_ref, routes_vmem, sems):
    shard_len = keys_ref.shape[0]
    q_rows = q_ref.shape[0]
    heads = q_ref.shape[1] // HD
    pairs = [
        (keys_ref, kv_ref.at[0]),
        (values_ref, kv_ref.at[1]),
        (keys_ref, left_ref.at[pl.ds(0, shard_len)]),
        (values_ref, left_ref.at[pl.ds(shard_len, shard_len)]),
        (routes_ref, routes_vmem),
    ]
    for h in range(heads):
        pairs.append(
            (
                q_ref.at[:, pl.ds(h * HD, HD)],
                left_ref.at[pl.ds(2 * shard_len + h * q_rows, q_rows)],
            )
        )
    fetch(pairs, sems)
    at = 2 * shard_len + heads * q_rows
    size = left_ref.shape[0] - at
    choices, tokens = routes_vmem.shape
    left_ref[at:] = jnp.zeros((size, HD), BF16)
    left_ref[at : at + choices, :tokens] = routes_vmem[...].astype(F32).astype(BF16)


def forward(own_ref, near_ref, out_ref):
    rows = out_ref.shape[1] - own_ref.shape[1]
    out_ref[:, :rows] = near_ref[:, near_ref.shape[1] - rows :]
    out_ref[:, rows:] = own_ref[...]


def spread(came_ref, message_ref):
    tail = came_ref[came_ref.shape[0] - ROUTE_ROWS :].astype(F32).astype(jnp.int32)
    _, choices, tokens = message_ref.shape
    message_ref[...] = jnp.broadcast_to(tail[:choices, :tokens][None], message_ref.shape)


def second(
    shard_len, q_rows,
    lengths_hbm, routes_hbm, gates_hbm,
    begin_ref, selector_ref, column_ref,
    lengths_ref, routes_ref, gates_ref, sems,
):
    pairs = [
        (lengths_hbm, lengths_ref),
        (routes_hbm, routes_ref),
        (gates_hbm, gates_ref),
    ]
    fetch(pairs, sems)
    routes = routes_ref[...]
    place = lax.broadcasted_iota(jnp.int32, begin_ref.shape, 0)
    qpos = (worked_on() + 1) * shard_len - q_rows + place
    begin = jnp.zeros(begin_ref.shape, jnp.int32)
    start = jnp.zeros((1, 1), jnp.int32)
    for j in range(lengths_ref.shape[1]):
        begin = jnp.where(start <= qpos, start, begin)
        start = start + lengths_ref[:, j : j + 1]
    begin_ref[...] = begin

    _, rows, tokens = selector_ref.shape
    capacity = 3
    row = lax.broadcasted_iota(jnp.int32, (rows, tokens), 0)
    named = [routes[k : k + 1, :] == row // capacity for k in range(2)]
    before = lax.broadcasted_iota(jnp.int32, (tokens, tokens), 0) < (
        lax.broadcasted_iota(jnp.int32, (tokens, tokens), 1)
    )
    either = (named[0] | named[1]).astype(F32).astype(BF16)
    ahead = jnp.dot(either, before.astype(F32).astype(BF16), preferred_element_type=F32)
    right = ahead == (row % capacity).astype(F32)
    diagonal = lax.broadcasted_iota(jnp.int32, (tokens, tokens), 0) == (
        lax.broadcasted_iota(jnp.int32, (tokens, tokens), 1)
    )
    for k in range(2):
        selector_ref[k] = (named[k] & right).astype(F32).astype(BF16)
        gate = jnp.where(diagonal, gates_ref[k : k + 1, :], F32(0))
        gate = jnp.sum(gate, axis=1, keepdims=True)
        column_ref[k] = jnp.broadcast_to(gate, column_ref.shape[1:])


def attend(begin_ref, routes_ref, came_ref, own_ref, near_ref, beyond_ref, out_ref):
    shard_len = own_ref.shape[1]
    q_rows = begin_ref.shape[0]
    heads = out_ref.shape[2] // HD
    me = worked_on()
    rows = heads * q_rows
    queries = came_ref[2 * shard_len : 2 * shard_len + rows]
    begin = jnp.concatenate([begin_ref[:, 0:1]] * heads, axis=0)
    place = lax.broadcasted_iota(jnp.int32, (rows, 1), 0) % q_rows
    qpos = (me + 1) * shard_len - q_rows + place
    parts = [(came_ref[:shard_len], came_ref[shard_len : 2 * shard_len])]
    parts += [(ref[0], ref[1]) for ref in (own_ref, near_ref, beyond_ref)]
    scores = []
    for d, (keys, _) in enumerate(parts):
        count = keys.shape[0]
        kpos = (me + 1 - d) * shard_len - count + lax.broadcasted_iota(jnp.int32, (1, count), 1)
        score = lax.dot_general(queries, keys, (((1,), (1,)), ((), ())), preferred_element_type=F32)
        allowed = kpos >= begin
        if d == 0:
            allowed = allowed & (kpos <= qpos)
        scores.append(jnp.where(allowed, score, F32(-1e30)))
    peak = functools.reduce(jnp.maximum, [jnp.max(s, axis=1, keepdims=True) for s in scores])
    total = jnp.zeros((rows, 1), F32)
    acc = jnp.zeros((rows, HD), F32)
    for score, (_, values) in zip(scores, parts):
        weight = jnp.exp((score - peak) * F32(HD**-0.5))
        total = total + jnp.sum(weight, axis=1, keepdims=True)
        acc = acc + jnp.dot(weight.astype(BF16), values, preferred_element_type=F32)
    attended = (acc / total).astype(BF16)
    wide = jnp.concatenate([attended[h * q_rows : (h + 1) * q_rows] for h in range(heads)], axis=1)

    blocks, _, tokens = routes_ref.shape
    experts = out_ref.shape[0]
    slots = out_ref.shape[1]
    spread = lax.broadcasted_iota(jnp.int32, (tokens, q_rows), 0) == (
        lax.broadcasted_iota(jnp.int32, (tokens, q_rows), 1) % tokens
    )
    block_of = lax.broadcasted_iota(jnp.int32, (blocks, q_rows), 1) // tokens
    in_block = lax.broadcasted_iota(jnp.int32, (blocks, q_rows), 0) == block_of
    expert_id = lax.broadcasted_iota(jnp.int32, (experts, q_rows), 0).astype(F32)
    named = jnp.zeros((experts, q_rows), jnp.bool_)
    for k in range(2):
        chosen = routes_ref[:, k, :].astype(F32).astype(BF16)
        by_block = jnp.dot(chosen, spread.astype(BF16), preferred_element_type=F32)
        flat = jnp.sum(jnp.where(in_block, by_block, 0.0), axis=0, keepdims=True)
        named = named | (flat == expert_id)
    r = lax.broadcasted_iota(jnp.int32, (q_rows, q_rows), 0)
    c = lax.broadcasted_iota(jnp.int32, (q_rows, q_rows), 1)
    earlier = (r // tokens == c // tokens) & (r < c)
    ahead = jnp.dot(named.astype(BF16), earlier.astype(BF16), preferred_element_type=F32)
    token_block = lax.broadcasted_iota(jnp.int32, (experts, q_rows), 1) // tokens
    slot = jnp.where(named, ahead * F32(blocks) + token_block.astype(F32), F32(-1))
    slot_id = lax.broadcasted_iota(jnp.int32, (slots, q_rows), 0).astype(F32)
    selector = jnp.concatenate(
        [(slot_id == slot[e : e + 1, :]).astype(F32) for e in range(experts)], axis=0
    ).astype(BF16)
    picked = jnp.dot(selector, wide, preferred_element_type=F32)
    out_ref[...] = picked.reshape(out_ref.shape).astype(BF16)


def pack(x_ref, out_ref):
    experts, _, chunk = x_ref.shape
    parts = [x_ref[e].astype(F32) for e in range(experts)]
    square = sum(jnp.sum(x * x, axis=1, keepdims=True) for x in parts)
    largest = functools.reduce(
        jnp.maximum, [jnp.max(jnp.abs(x), axis=1, keepdims=True) for x in parts]
    )
    largest = jnp.maximum(largest, F32(1e-30))
    up = F32(FIXED) / largest
    for e, x in enumerate(parts):
        fixed = jnp.round(x * up).astype(jnp.int32)
        out_ref[:, e * chunk : (e + 1) * chunk] = fixed.astype(jnp.int16)
    down = largest * F32(1 / FIXED) * lax.rsqrt(square / F32(experts * chunk) + F32(1e-05))
    power = jnp.floor(jnp.log2(down))
    digits = jnp.round(down * jnp.exp2(-power) * F32(DIGITS))
    tail = (x_ref.shape[1], out_ref.shape[1] - experts * chunk)
    lane = lax.broadcasted_iota(jnp.int32, tail, 1)
    factor = jnp.where(lane == 0, digits, jnp.where(lane == 1, power, F32(0)))
    out_ref[:, experts * chunk :] = factor.astype(jnp.int32).astype(jnp.int16)


def project(chunks, x_ref, w_ref, out_ref, w_vmem, sems):
    seq_count = x_ref.shape[0]
    depth = w_vmem.shape[0]
    chunk = depth // chunks

    def copy(e):
        at = pl.ds(e * chunk, chunk)
        return pltpu.make_async_copy(w_ref.at[0, at], w_vmem.at[at], sems.at[e])

    def rows(lo, size):
        part = [x_ref[s - 1, :, lo : lo + size].astype(jnp.int32) for s in order]
        return jnp.concatenate(part, axis=0).astype(F32)

    order = [s or seq_count for s in range(seq_count)]

    for e in range(chunks):
        copy(e).start()
    factor = rows(depth, HD)
    factor = factor[:, 0:1] * F32(1 / DIGITS) * jnp.exp2(factor[:, 1:2])
    acc = jnp.zeros((seq_count * x_ref.shape[1], w_vmem.shape[1]), F32)
    for e in range(chunks):
        x = rows(e * chunk, chunk).astype(BF16)
        copy(e).wait()
        acc = acc + jnp.dot(
            x, w_vmem[e * chunk : (e + 1) * chunk], preferred_element_type=F32
        )
    upper = acc * factor
    act = (upper / (1.0 + jnp.exp(-upper))).reshape(-1, PEERS, upper.shape[1])
    tiles = upper.shape[1] // HD
    parts = [act[:, :, j * HD : (j + 1) * HD] for j in range(tiles)]
    parts += [jnp.zeros_like(parts[0])] * (PEERS - tiles)
    turned = jnp.swapaxes(jnp.stack(parts, axis=1), 1, 2).astype(BF16)
    slots = out_ref.shape[1] // PEERS
    for s in range(seq_count):
        for c in range(slots):
            at = pl.ds(c * PEERS, PEERS)
            out_ref[s * PEERS : (s + 1) * PEERS, at] = turned[s * slots + c]


def mix(back_ref, selector_ref, column_ref, out_ref):
    seq_count = back_ref.shape[0] // PEERS
    units = out_ref.shape[1] // seq_count
    tiles = units // HD
    rows = selector_ref.shape[1]
    for s in range(seq_count):
        back = back_ref[s * PEERS : (s + 1) * PEERS].astype(F32)
        back = jnp.swapaxes(back.reshape(rows // PEERS, PEERS, PEERS, HD), 1, 2)
        wide = [back[:, j].reshape(rows, HD) for j in range(tiles)]
        wide = jnp.concatenate(wide, axis=1).astype(BF16)
        both = F32(0)
        for k in range(2):
            picked = lax.dot_general(
                selector_ref[k], wide, (((0,), (0,)), ((), ())), preferred_element_type=F32
            )
            both = both + picked * column_ref[k, :, 0:1]
        out_ref[:, s * units : (s + 1) * units] = both.astype(BF16)


def shards(queries, keys, values, lengths, routes, gates, w_up):
    q_rows, width = queries.shape
    shard_len = keys.shape[0]
    seq_count = lax.axis_size("seq")
    expert_count = lax.axis_size("expert")
    capacity = 3
    tok_count = routes.shape[0]
    per_expert = expert_count * capacity
    reach = LONGEST + shard_len
    reach = reach - (shard_len - q_rows)

    heads = width // HD
    keys, values, queries, lengths, routes, gates = (
        pltpu.with_memory_space_constraint(x, pltpu.HBM)
        for x in (keys, values, queries, lengths.reshape(1, -1), routes.T, gates.T)
    )
    hbm = pl.BlockSpec(memory_space=pltpu.HBM)
    small = pltpu.CompilerParams(vmem_limit_bytes=8 << 20)
    left_rows = 2 * shard_len + heads * q_rows + ROUTE_ROWS
    own, left = pl.pallas_call(
        first,
        out_shape=(
            jax.ShapeDtypeStruct((2, shard_len, HD), BF16),
            jax.ShapeDtypeStruct((left_rows, HD), BF16),
        ),
        in_specs=[hbm] * 4,
        out_specs=(VMEM,) * 2,
        scratch_shapes=[
            pltpu.VMEM(routes.shape, jnp.int32),
            pltpu.SemaphoreType.DMA((5 + heads,)),
        ],
        compiler_params=small,
        name="first",
    )(keys, values, queries, routes)
    begin, selectors, columns = pl.pallas_call(
        functools.partial(second, shard_len, q_rows),
        out_shape=(
            jax.ShapeDtypeStruct((q_rows, HD), jnp.int32),
            jax.ShapeDtypeStruct((2, per_expert, tok_count), BF16),
            jax.ShapeDtypeStruct((2, tok_count, HD), F32),
        ),
        in_specs=[hbm] * 3,
        out_specs=(VMEM,) * 3,
        scratch_shapes=[
            pltpu.VMEM(lengths.shape, jnp.int32),
            pltpu.VMEM(routes.shape, jnp.int32),
            pltpu.VMEM(gates.shape, F32),
            pltpu.SemaphoreType.DMA((3,)),
        ],
        compiler_params=small,
        cost_estimate=pl.CostEstimate(flops=4_000_000, bytes_accessed=200_000, transcendentals=0),
        name="second",
    )(lengths, routes, gates)

    def shifted(x, by):
        return lax.ppermute(x, "seq", [(i, (i + by) % seq_count) for i in range(seq_count)])

    near = shifted(own, 1)
    came = shifted(left, -1)
    beyond = pl.pallas_call(
        forward,
        out_shape=jax.ShapeDtypeStruct((2, reach - 3 * shard_len, HD), BF16),
        in_specs=[VMEM] * 2,
        out_specs=VMEM,
        compiler_params=small,
        name="forward",
    )(own, near)
    beyond = shifted(beyond, 2)
    message = pl.pallas_call(
        spread,
        out_shape=jax.ShapeDtypeStruct((expert_count, 2, tok_count), jnp.int32),
        in_specs=[VMEM],
        out_specs=VMEM,
        compiler_params=small,
        name="spread",
    )(came)
    row_routes = exchange(message, "expert")

    outgoing = pl.pallas_call(
        attend,
        out_shape=jax.ShapeDtypeStruct((expert_count, per_expert, width), BF16),
        in_specs=[VMEM] * 6,
        out_specs=VMEM,
        compiler_params=pltpu.CompilerParams(vmem_limit_bytes=24 << 20),
        name="attend",
    )(begin, row_routes, came, own, near, beyond)
    landed = exchange(outgoing, "expert")
    packed = pl.pallas_call(
        pack,
        out_shape=jax.ShapeDtypeStruct((per_expert, expert_count * width + HD), jnp.int16),
        in_specs=[VMEM],
        out_specs=VMEM,
        compiler_params=pltpu.CompilerParams(vmem_limit_bytes=16 << 20),
        name="pack",
    )(landed)
    incoming = lax.all_gather(packed, "seq")
    act = pl.pallas_call(
        functools.partial(project, expert_count),
        out_shape=jax.ShapeDtypeStruct((seq_count * expert_count, per_expert, HD), BF16),
        in_specs=[VMEM, pl.BlockSpec(memory_space=pltpu.HBM)],
        out_specs=VMEM,
        scratch_shapes=[
            pltpu.VMEM(w_up.shape[1:], BF16),
            pltpu.SemaphoreType.DMA((expert_count,)),
        ],
        compiler_params=pltpu.CompilerParams(vmem_limit_bytes=32 << 20),
        name="project",
    )(incoming, pltpu.with_memory_space_constraint(w_up, pltpu.HBM))
    back = exchange(act, ("seq", "expert"))
    return pl.pallas_call(
        mix,
        out_shape=jax.ShapeDtypeStruct((tok_count, seq_count * w_up.shape[2]), BF16),
        in_specs=[VMEM] * 3,
        out_specs=VMEM,
        compiler_params=pltpu.CompilerParams(vmem_limit_bytes=16 << 20),
        name="mix",
    )(back, selectors, columns)


def solution(mesh):
    placed = (
        P(("dp", "seq"), "expert"),
        P(("dp", "seq"), "expert"),
        P(("dp", "seq"), "expert"),
        P("dp"),
        P(("dp", "seq", "expert"), None),
        P(("dp", "seq", "expert"), None),
        P("expert", None, "seq"),
    )

    return jax.shard_map(
        shards,
        mesh=mesh,
        in_specs=placed,
        out_specs=P(("dp", "seq", "expert"), None),
        check_vma=False,
    )
```

```python
import functools

import jax
import jax.numpy as jnp
from jax import lax
from jax.experimental import pallas as pl
from jax.experimental.pallas import tpu as pltpu
from jax.sharding import PartitionSpec as P


HD = 128
LONGEST = 1024
FIXED = 32767
DIGITS = 8192
PEERS = 8
ROUTE_ROWS = 16
F32 = jnp.float32
BF16 = jnp.bfloat16
VMEM = pl.BlockSpec(memory_space=pltpu.VMEM)


def exchange(x, axis):
    return lax.all_to_all(x, axis, split_axis=0, concat_axis=0, tiled=True)


def worked_on():
    return lax.rem(lax.axis_index("seq") + 1, lax.axis_size("seq"))


def fetch(pairs, sems):
    copies = [pltpu.make_async_copy(a, b, sems.at[i]) for i, (a, b) in enumerate(pairs)]
    for copy in copies:
        copy.start()
    for copy in copies:
        copy.wait()


def first(keys_ref, values_ref, q_ref, routes_ref, kv_ref, left_ref, routes_vmem, sems):
    shard_len = keys_ref.shape[0]
    q_rows = q_ref.shape[0]
    heads = q_ref.shape[1] // HD
    pairs = [
        (keys_ref, kv_ref.at[0]),
        (values_ref, kv_ref.at[1]),
        (keys_ref, left_ref.at[pl.ds(0, shard_len)]),
        (values_ref, left_ref.at[pl.ds(shard_len, shard_len)]),
        (routes_ref, routes_vmem),
    ]
    for h in range(heads):
        pairs.append(
            (
                q_ref.at[:, pl.ds(h * HD, HD)],
                left_ref.at[pl.ds(2 * shard_len + h * q_rows, q_rows)],
            )
        )
    fetch(pairs, sems)
    at = 2 * shard_len + heads * q_rows
    size = left_ref.shape[0] - at
    choices, tokens = routes_vmem.shape
    left_ref[at:] = jnp.zeros((size, HD), BF16)
    left_ref[at : at + choices, :tokens] = routes_vmem[...].astype(F32).astype(BF16)


def forward(own_ref, near_ref, out_ref):
    rows = out_ref.shape[1] - own_ref.shape[1]
    out_ref[:, :rows] = near_ref[:, near_ref.shape[1] - rows :]
    out_ref[:, rows:] = own_ref[...]


def spread(came_ref, message_ref):
    tail = came_ref[came_ref.shape[0] - ROUTE_ROWS :].astype(F32).astype(jnp.int32)
    _, choices, tokens = message_ref.shape
    message_ref[...] = jnp.broadcast_to(tail[:choices, :tokens][None], message_ref.shape)


def second(
    shard_len, q_rows,
    lengths_hbm, routes_hbm, gates_hbm,
    begin_ref, selector_ref, column_ref,
    lengths_ref, routes_ref, gates_ref, sems,
):
    pairs = [
        (lengths_hbm, lengths_ref),
        (routes_hbm, routes_ref),
        (gates_hbm, gates_ref),
    ]
    fetch(pairs, sems)
    routes = routes_ref[...]
    place = lax.broadcasted_iota(jnp.int32, begin_ref.shape, 0)
    qpos = (worked_on() + 1) * shard_len - q_rows + place
    begin = jnp.zeros(begin_ref.shape, jnp.int32)
    start = jnp.zeros((1, 1), jnp.int32)
    for j in range(lengths_ref.shape[1]):
        begin = jnp.where(start <= qpos, start, begin)
        start = start + lengths_ref[:, j : j + 1]
    begin_ref[...] = begin

    _, rows, tokens = selector_ref.shape
    capacity = 3
    row = lax.broadcasted_iota(jnp.int32, (rows, tokens), 0)
    named = [routes[k : k + 1, :] == row // capacity for k in range(2)]
    before = lax.broadcasted_iota(jnp.int32, (tokens, tokens), 0) < (
        lax.broadcasted_iota(jnp.int32, (tokens, tokens), 1)
    )
    either = (named[0] | named[1]).astype(F32).astype(BF16)
    ahead = jnp.dot(either, before.astype(F32).astype(BF16), preferred_element_type=F32)
    right = ahead == (row % capacity).astype(F32)
    diagonal = lax.broadcasted_iota(jnp.int32, (tokens, tokens), 0) == (
        lax.broadcasted_iota(jnp.int32, (tokens, tokens), 1)
    )
    for k in range(2):
        selector_ref[k] = (named[k] & right).astype(F32).astype(BF16)
        gate = jnp.where(diagonal, gates_ref[k : k + 1, :], F32(0))
        gate = jnp.sum(gate, axis=1, keepdims=True)
        column_ref[k] = jnp.broadcast_to(gate, column_ref.shape[1:])


def attend(begin_ref, came_ref, own_ref, near_ref, beyond_ref, out_ref):
    shard_len = own_ref.shape[1]
    q_rows = begin_ref.shape[0]
    heads = out_ref.shape[1] // HD
    me = worked_on()
    rows = heads * q_rows
    queries = came_ref[2 * shard_len : 2 * shard_len + rows]
    begin = jnp.concatenate([begin_ref[:, 0:1]] * heads, axis=0)
    place = lax.broadcasted_iota(jnp.int32, (rows, 1), 0) % q_rows
    qpos = (me + 1) * shard_len - q_rows + place
    parts = [(came_ref[:shard_len], came_ref[shard_len : 2 * shard_len])]
    parts += [(ref[0], ref[1]) for ref in (own_ref, near_ref, beyond_ref)]
    scores = []
    for d, (keys, _) in enumerate(parts):
        count = keys.shape[0]
        kpos = (me + 1 - d) * shard_len - count + lax.broadcasted_iota(jnp.int32, (1, count), 1)
        score = lax.dot_general(queries, keys, (((1,), (1,)), ((), ())), preferred_element_type=F32)
        allowed = kpos >= begin
        if d == 0:
            allowed = allowed & (kpos <= qpos)
        scores.append(jnp.where(allowed, score, F32(-1e30)))
    peak = functools.reduce(jnp.maximum, [jnp.max(s, axis=1, keepdims=True) for s in scores])
    total = jnp.zeros((rows, 1), F32)
    acc = jnp.zeros((rows, HD), F32)
    for score, (_, values) in zip(scores, parts):
        weight = jnp.exp((score - peak) * F32(HD**-0.5))
        total = total + jnp.sum(weight, axis=1, keepdims=True)
        acc = acc + jnp.dot(weight.astype(BF16), values, preferred_element_type=F32)
    attended = (acc / total).astype(BF16)
    for h in range(heads):
        out_ref[:, h * HD : (h + 1) * HD] = attended[h * q_rows : (h + 1) * q_rows]


def select(wide_ref, routes_ref, out_ref):
    q_rows = wide_ref.shape[0]
    blocks, _, tokens = routes_ref.shape
    experts = out_ref.shape[0]
    slots = out_ref.shape[1]
    spread = lax.broadcasted_iota(jnp.int32, (tokens, q_rows), 0) == (
        lax.broadcasted_iota(jnp.int32, (tokens, q_rows), 1) % tokens
    )
    block_of = lax.broadcasted_iota(jnp.int32, (blocks, q_rows), 1) // tokens
    in_block = lax.broadcasted_iota(jnp.int32, (blocks, q_rows), 0) == block_of
    expert_id = lax.broadcasted_iota(jnp.int32, (experts, q_rows), 0).astype(F32)
    named = jnp.zeros((experts, q_rows), jnp.bool_)
    for k in range(2):
        chosen = routes_ref[:, k, :].astype(F32).astype(BF16)
        by_block = jnp.dot(chosen, spread.astype(BF16), preferred_element_type=F32)
        flat = jnp.sum(jnp.where(in_block, by_block, 0.0), axis=0, keepdims=True)
        named = named | (flat == expert_id)
    r = lax.broadcasted_iota(jnp.int32, (q_rows, q_rows), 0)
    c = lax.broadcasted_iota(jnp.int32, (q_rows, q_rows), 1)
    earlier = (r // tokens == c // tokens) & (r < c)
    ahead = jnp.dot(named.astype(BF16), earlier.astype(BF16), preferred_element_type=F32)
    token_block = lax.broadcasted_iota(jnp.int32, (experts, q_rows), 1) // tokens
    slot = jnp.where(named, ahead * F32(blocks) + token_block.astype(F32), F32(-1))
    slot_id = lax.broadcasted_iota(jnp.int32, (slots, q_rows), 0).astype(F32)
    selector = jnp.concatenate(
        [(slot_id == slot[e : e + 1, :]).astype(F32) for e in range(experts)], axis=0
    ).astype(BF16)
    picked = jnp.dot(selector, wide_ref[...], preferred_element_type=F32)
    out_ref[...] = picked.reshape(out_ref.shape).astype(BF16)


def pack(x_ref, out_ref):
    experts, _, chunk = x_ref.shape
    parts = [x_ref[e].astype(F32) for e in range(experts)]
    square = sum(jnp.sum(x * x, axis=1, keepdims=True) for x in parts)
    largest = functools.reduce(
        jnp.maximum, [jnp.max(jnp.abs(x), axis=1, keepdims=True) for x in parts]
    )
    largest = jnp.maximum(largest, F32(1e-30))
    up = F32(FIXED) / largest
    for e, x in enumerate(parts):
        fixed = jnp.round(x * up).astype(jnp.int32)
        out_ref[:, e * chunk : (e + 1) * chunk] = fixed.astype(jnp.int16)
    down = largest * F32(1 / FIXED) * lax.rsqrt(square / F32(experts * chunk) + F32(1e-05))
    power = jnp.floor(jnp.log2(down))
    digits = jnp.round(down * jnp.exp2(-power) * F32(DIGITS))
    tail = (x_ref.shape[1], out_ref.shape[1] - experts * chunk)
    lane = lax.broadcasted_iota(jnp.int32, tail, 1)
    factor = jnp.where(lane == 0, digits, jnp.where(lane == 1, power, F32(0)))
    out_ref[:, experts * chunk :] = factor.astype(jnp.int32).astype(jnp.int16)


def project(chunks, x_ref, w_ref, out_ref, w_vmem, sems):
    seq_count = x_ref.shape[0]
    depth = w_vmem.shape[0]
    chunk = depth // chunks

    def copy(e):
        at = pl.ds(e * chunk, chunk)
        return pltpu.make_async_copy(w_ref.at[0, at], w_vmem.at[at], sems.at[e])

    def rows(lo, size):
        part = [x_ref[s - 1, :, lo : lo + size].astype(jnp.int32) for s in order]
        return jnp.concatenate(part, axis=0).astype(F32)

    order = [s or seq_count for s in range(seq_count)]

    for e in range(chunks):
        copy(e).start()
    factor = rows(depth, HD)
    factor = factor[:, 0:1] * F32(1 / DIGITS) * jnp.exp2(factor[:, 1:2])
    acc = jnp.zeros((seq_count * x_ref.shape[1], w_vmem.shape[1]), F32)
    for e in range(chunks):
        x = rows(e * chunk, chunk).astype(BF16)
        copy(e).wait()
        acc = acc + jnp.dot(
            x, w_vmem[e * chunk : (e + 1) * chunk], preferred_element_type=F32
        )
    upper = acc * factor
    act = (upper / (1.0 + jnp.exp(-upper))).reshape(-1, PEERS, upper.shape[1])
    tiles = upper.shape[1] // HD
    parts = [act[:, :, j * HD : (j + 1) * HD] for j in range(tiles)]
    parts += [jnp.zeros_like(parts[0])] * (PEERS - tiles)
    turned = jnp.swapaxes(jnp.stack(parts, axis=1), 1, 2).astype(BF16)
    slots = out_ref.shape[1] // PEERS
    for s in range(seq_count):
        for c in range(slots):
            at = pl.ds(c * PEERS, PEERS)
            out_ref[s * PEERS : (s + 1) * PEERS, at] = turned[s * slots + c]


def mix(back_ref, selector_ref, column_ref, out_ref):
    seq_count = back_ref.shape[0] // PEERS
    units = out_ref.shape[1] // seq_count
    tiles = units // HD
    rows = selector_ref.shape[1]
    for s in range(seq_count):
        back = back_ref[s * PEERS : (s + 1) * PEERS].astype(F32)
        back = jnp.swapaxes(back.reshape(rows // PEERS, PEERS, PEERS, HD), 1, 2)
        wide = [back[:, j].reshape(rows, HD) for j in range(tiles)]
        wide = jnp.concatenate(wide, axis=1).astype(BF16)
        both = F32(0)
        for k in range(2):
            picked = lax.dot_general(
                selector_ref[k], wide, (((0,), (0,)), ((), ())), preferred_element_type=F32
            )
            both = both + picked * column_ref[k, :, 0:1]
        out_ref[:, s * units : (s + 1) * units] = both.astype(BF16)


def shards(queries, keys, values, lengths, routes, gates, w_up):
    q_rows, width = queries.shape
    shard_len = keys.shape[0]
    seq_count = lax.axis_size("seq")
    expert_count = lax.axis_size("expert")
    capacity = 3
    tok_count = routes.shape[0]
    per_expert = expert_count * capacity
    reach = LONGEST + shard_len
    reach = reach - (shard_len - q_rows)

    heads = width // HD
    keys, values, queries, lengths, routes, gates = (
        pltpu.with_memory_space_constraint(x, pltpu.HBM)
        for x in (keys, values, queries, lengths.reshape(1, -1), routes.T, gates.T)
    )
    hbm = pl.BlockSpec(memory_space=pltpu.HBM)
    small = pltpu.CompilerParams(vmem_limit_bytes=8 << 20)
    left_rows = 2 * shard_len + heads * q_rows + ROUTE_ROWS
    own, left = pl.pallas_call(
        first,
        out_shape=(
            jax.ShapeDtypeStruct((2, shard_len, HD), BF16),
            jax.ShapeDtypeStruct((left_rows, HD), BF16),
        ),
        in_specs=[hbm] * 4,
        out_specs=(VMEM,) * 2,
        scratch_shapes=[
            pltpu.VMEM(routes.shape, jnp.int32),
            pltpu.SemaphoreType.DMA((5 + heads,)),
        ],
        compiler_params=small,
        name="first",
    )(keys, values, queries, routes)
    bounds = pl.pallas_call(
        functools.partial(second, shard_len, q_rows),
        out_shape=(
            jax.ShapeDtypeStruct((q_rows, HD), jnp.int32),
            jax.ShapeDtypeStruct((2, per_expert, tok_count), BF16),
            jax.ShapeDtypeStruct((2, tok_count, HD), F32),
        ),
        in_specs=[hbm] * 3,
        out_specs=(VMEM,) * 3,
        scratch_shapes=[
            pltpu.VMEM(lengths.shape, jnp.int32),
            pltpu.VMEM(routes.shape, jnp.int32),
            pltpu.VMEM(gates.shape, F32),
            pltpu.SemaphoreType.DMA((3,)),
        ],
        compiler_params=small,
        cost_estimate=pl.CostEstimate(flops=4_000_000, bytes_accessed=200_000, transcendentals=0),
        name="second",
    )(lengths, routes, gates)
    begin, selectors, columns = bounds

    def shifted(x, by):
        return lax.ppermute(x, "seq", [(i, (i + by) % seq_count) for i in range(seq_count)])

    near = shifted(own, 1)
    came = shifted(left, -1)
    beyond = pl.pallas_call(
        forward,
        out_shape=jax.ShapeDtypeStruct((2, reach - 3 * shard_len, HD), BF16),
        in_specs=[VMEM] * 2,
        out_specs=VMEM,
        compiler_params=small,
        name="forward",
    )(own, near)
    beyond = shifted(beyond, 2)
    message = pl.pallas_call(
        spread,
        out_shape=jax.ShapeDtypeStruct((expert_count, 2, tok_count), jnp.int32),
        in_specs=[VMEM],
        out_specs=VMEM,
        compiler_params=small,
        name="spread",
    )(came)
    row_routes = exchange(message, "expert")

    attended = pl.pallas_call(
        attend,
        out_shape=jax.ShapeDtypeStruct((q_rows, width), BF16),
        in_specs=[VMEM] * 5,
        out_specs=VMEM,
        compiler_params=pltpu.CompilerParams(vmem_limit_bytes=24 << 20),
        cost_estimate=pl.CostEstimate(
            flops=4 * heads * q_rows * reach * HD, bytes_accessed=0, transcendentals=0
        ),
        name="attend",
    )(begin, came, own, near, beyond)
    outgoing = pl.pallas_call(
        select,
        out_shape=jax.ShapeDtypeStruct((expert_count, per_expert, width), BF16),
        in_specs=[VMEM] * 2,
        out_specs=VMEM,
        compiler_params=small,
        name="select",
    )(attended, row_routes)
    landed = exchange(outgoing, "expert")
    packed = pl.pallas_call(
        pack,
        out_shape=jax.ShapeDtypeStruct((per_expert, expert_count * width + HD), jnp.int16),
        in_specs=[VMEM],
        out_specs=VMEM,
        compiler_params=pltpu.CompilerParams(vmem_limit_bytes=16 << 20),
        name="pack",
    )(landed)
    incoming = lax.all_gather(packed, "seq")
    act = pl.pallas_call(
        functools.partial(project, expert_count),
        out_shape=jax.ShapeDtypeStruct((seq_count * expert_count, per_expert, HD), BF16),
        in_specs=[VMEM, pl.BlockSpec(memory_space=pltpu.HBM)],
        out_specs=VMEM,
        scratch_shapes=[
            pltpu.VMEM(w_up.shape[1:], BF16),
            pltpu.SemaphoreType.DMA((expert_count,)),
        ],
        compiler_params=pltpu.CompilerParams(vmem_limit_bytes=32 << 20),
        name="project",
    )(incoming, pltpu.with_memory_space_constraint(w_up, pltpu.HBM))
    back = exchange(act, ("seq", "expert"))
    return pl.pallas_call(
        mix,
        out_shape=jax.ShapeDtypeStruct((tok_count, seq_count * w_up.shape[2]), BF16),
        in_specs=[VMEM] * 3,
        out_specs=VMEM,
        compiler_params=pltpu.CompilerParams(vmem_limit_bytes=16 << 20),
        name="mix",
    )(back, selectors, columns)


def solution(mesh):
    placed = (
        P(("dp", "seq"), "expert"),
        P(("dp", "seq"), "expert"),
        P(("dp", "seq"), "expert"),
        P("dp"),
        P(("dp", "seq", "expert"), None),
        P(("dp", "seq", "expert"), None),
        P("expert", None, "seq"),
    )

    return jax.shard_map(
        shards,
        mesh=mesh,
        in_specs=placed,
        out_specs=P(("dp", "seq", "expert"), None),
        check_vma=False,
    )
```

```python
import functools

import jax
import jax.numpy as jnp
from jax import lax
from jax.experimental import pallas as pl
from jax.experimental.pallas import tpu as pltpu
from jax.sharding import PartitionSpec as P


HD = 128
LONGEST = 1024
FIXED = 32767
DIGITS = 8192
PEERS = 8
ROUTE_ROWS = 16
F32 = jnp.float32
BF16 = jnp.bfloat16
VMEM = pl.BlockSpec(memory_space=pltpu.VMEM)


def exchange(x, axis):
    return lax.all_to_all(x, axis, split_axis=0, concat_axis=0, tiled=True)


def worked_on():
    return lax.rem(lax.axis_index("seq") + 1, lax.axis_size("seq"))


def fetch(pairs, sems):
    copies = [pltpu.make_async_copy(a, b, sems.at[i]) for i, (a, b) in enumerate(pairs)]
    for copy in copies:
        copy.start()
    for copy in copies:
        copy.wait()


def first(keys_ref, values_ref, q_ref, routes_ref, kv_ref, left_ref, routes_vmem, sems):
    shard_len = keys_ref.shape[0]
    q_rows = q_ref.shape[0]
    heads = q_ref.shape[1] // HD
    pairs = [
        (keys_ref, kv_ref.at[0]),
        (values_ref, kv_ref.at[1]),
        (keys_ref, left_ref.at[pl.ds(0, shard_len)]),
        (values_ref, left_ref.at[pl.ds(shard_len, shard_len)]),
        (routes_ref, routes_vmem),
    ]
    for h in range(heads):
        pairs.append(
            (
                q_ref.at[:, pl.ds(h * HD, HD)],
                left_ref.at[pl.ds(2 * shard_len + h * q_rows, q_rows)],
            )
        )
    fetch(pairs, sems)
    at = 2 * shard_len + heads * q_rows
    size = left_ref.shape[0] - at
    choices, tokens = routes_vmem.shape
    left_ref[at:] = jnp.zeros((size, HD), BF16)
    left_ref[at : at + choices, :tokens] = routes_vmem[...].astype(F32).astype(BF16)


def forward(own_ref, near_ref, out_ref):
    rows = out_ref.shape[1] - own_ref.shape[1]
    out_ref[:, :rows] = near_ref[:, near_ref.shape[1] - rows :]
    out_ref[:, rows:] = own_ref[...]


def spread(came_ref, message_ref):
    tail = came_ref[came_ref.shape[0] - ROUTE_ROWS :].astype(F32).astype(jnp.int32)
    _, choices, tokens = message_ref.shape
    message_ref[...] = jnp.broadcast_to(tail[:choices, :tokens][None], message_ref.shape)


def second(
    shard_len, q_rows,
    lengths_hbm, routes_hbm, gates_hbm,
    begin_ref, selector_ref, column_ref,
    lengths_ref, routes_ref, gates_ref, sems,
):
    pairs = [
        (lengths_hbm, lengths_ref),
        (routes_hbm, routes_ref),
        (gates_hbm, gates_ref),
    ]
    fetch(pairs, sems)
    routes = routes_ref[...]
    place = lax.broadcasted_iota(jnp.int32, begin_ref.shape, 0)
    qpos = (worked_on() + 1) * shard_len - q_rows + place
    begin = jnp.zeros(begin_ref.shape, jnp.int32)
    start = jnp.zeros((1, 1), jnp.int32)
    for j in range(lengths_ref.shape[1]):
        begin = jnp.where(start <= qpos, start, begin)
        start = start + lengths_ref[:, j : j + 1]
    begin_ref[...] = begin

    rows, tokens = selector_ref.shape[0], selector_ref.shape[1] // 2
    capacity = 3
    row = lax.broadcasted_iota(jnp.int32, (rows, tokens), 0)
    named = [routes[k : k + 1, :] == row // capacity for k in range(2)]
    before = lax.broadcasted_iota(jnp.int32, (tokens, tokens), 0) < (
        lax.broadcasted_iota(jnp.int32, (tokens, tokens), 1)
    )
    either = (named[0] | named[1]).astype(F32).astype(BF16)
    ahead = jnp.dot(either, before.astype(F32).astype(BF16), preferred_element_type=F32)
    right = ahead == (row % capacity).astype(F32)
    diagonal = lax.broadcasted_iota(jnp.int32, (tokens, tokens), 0) == (
        lax.broadcasted_iota(jnp.int32, (tokens, tokens), 1)
    )
    for k in range(2):
        chosen = (named[k] & right).astype(F32).astype(BF16)
        selector_ref[:, k * tokens : (k + 1) * tokens] = chosen
        gate = jnp.where(diagonal, gates_ref[k : k + 1, :], F32(0))
        gate = jnp.sum(gate, axis=1, keepdims=True)
        column_ref[k] = jnp.broadcast_to(gate, column_ref.shape[1:])


def attend(begin_ref, came_ref, own_ref, near_ref, beyond_ref, out_ref):
    shard_len = own_ref.shape[1]
    q_rows = begin_ref.shape[0]
    heads = out_ref.shape[1] // HD
    me = worked_on()
    rows = heads * q_rows
    queries = came_ref[2 * shard_len : 2 * shard_len + rows]
    begin = jnp.concatenate([begin_ref[:, 0:1]] * heads, axis=0)
    place = lax.broadcasted_iota(jnp.int32, (rows, 1), 0) % q_rows
    qpos = (me + 1) * shard_len - q_rows + place
    parts = [(came_ref[:shard_len], came_ref[shard_len : 2 * shard_len])]
    parts += [(ref[0], ref[1]) for ref in (own_ref, near_ref, beyond_ref)]
    scores = []
    for d, (keys, _) in enumerate(parts):
        count = keys.shape[0]
        kpos = (me + 1 - d) * shard_len - count + lax.broadcasted_iota(jnp.int32, (1, count), 1)
        score = lax.dot_general(queries, keys, (((1,), (1,)), ((), ())), preferred_element_type=F32)
        allowed = kpos >= begin
        if d == 0:
            allowed = allowed & (kpos <= qpos)
        scores.append(jnp.where(allowed, score, F32(-1e30)))
    peak = functools.reduce(jnp.maximum, [jnp.max(s, axis=1, keepdims=True) for s in scores])
    total = jnp.zeros((rows, 1), F32)
    acc = jnp.zeros((rows, HD), F32)
    for score, (_, values) in zip(scores, parts):
        weight = jnp.exp((score - peak) * F32(HD**-0.5))
        total = total + jnp.sum(weight, axis=1, keepdims=True)
        acc = acc + jnp.dot(weight.astype(BF16), values, preferred_element_type=F32)
    attended = (acc / total).astype(BF16)
    for h in range(heads):
        out_ref[:, h * HD : (h + 1) * HD] = attended[h * q_rows : (h + 1) * q_rows]


def select(wide_ref, routes_ref, out_ref):
    q_rows = wide_ref.shape[0]
    blocks, _, tokens = routes_ref.shape
    experts = out_ref.shape[0]
    slots = out_ref.shape[1]
    spread = lax.broadcasted_iota(jnp.int32, (tokens, q_rows), 0) == (
        lax.broadcasted_iota(jnp.int32, (tokens, q_rows), 1) % tokens
    )
    block_of = lax.broadcasted_iota(jnp.int32, (blocks, q_rows), 1) // tokens
    in_block = lax.broadcasted_iota(jnp.int32, (blocks, q_rows), 0) == block_of
    expert_id = lax.broadcasted_iota(jnp.int32, (experts, q_rows), 0).astype(F32)
    named = jnp.zeros((experts, q_rows), jnp.bool_)
    for k in range(2):
        chosen = routes_ref[:, k, :].astype(F32).astype(BF16)
        by_block = jnp.dot(chosen, spread.astype(BF16), preferred_element_type=F32)
        flat = jnp.sum(jnp.where(in_block, by_block, 0.0), axis=0, keepdims=True)
        named = named | (flat == expert_id)
    r = lax.broadcasted_iota(jnp.int32, (q_rows, q_rows), 0)
    c = lax.broadcasted_iota(jnp.int32, (q_rows, q_rows), 1)
    earlier = (r // tokens == c // tokens) & (r < c)
    ahead = jnp.dot(named.astype(BF16), earlier.astype(BF16), preferred_element_type=F32)
    token_block = lax.broadcasted_iota(jnp.int32, (experts, q_rows), 1) // tokens
    slot = jnp.where(named, ahead * F32(blocks) + token_block.astype(F32), F32(-1))
    slot_id = lax.broadcasted_iota(jnp.int32, (slots, q_rows), 0).astype(F32)
    selector = jnp.concatenate(
        [(slot_id == slot[e : e + 1, :]).astype(F32) for e in range(experts)], axis=0
    ).astype(BF16)
    picked = jnp.dot(selector, wide_ref[...], preferred_element_type=F32)
    out_ref[...] = picked.reshape(out_ref.shape).astype(BF16)


def pack(x_ref, out_ref):
    experts, _, chunk = x_ref.shape
    parts = [x_ref[e].astype(F32) for e in range(experts)]
    square = sum(jnp.sum(x * x, axis=1, keepdims=True) for x in parts)
    largest = functools.reduce(
        jnp.maximum, [jnp.max(jnp.abs(x), axis=1, keepdims=True) for x in parts]
    )
    largest = jnp.maximum(largest, F32(1e-30))
    up = F32(FIXED) / largest
    for e, x in enumerate(parts):
        fixed = jnp.round(x * up).astype(jnp.int32)
        out_ref[:, e * chunk : (e + 1) * chunk] = fixed.astype(jnp.int16)
    down = largest * F32(1 / FIXED) * lax.rsqrt(square / F32(experts * chunk) + F32(1e-05))
    power = jnp.floor(jnp.log2(down))
    digits = jnp.round(down * jnp.exp2(-power) * F32(DIGITS))
    tail = (x_ref.shape[1], out_ref.shape[1] - experts * chunk)
    lane = lax.broadcasted_iota(jnp.int32, tail, 1)
    factor = jnp.where(lane == 0, digits, jnp.where(lane == 1, power, F32(0)))
    out_ref[:, experts * chunk :] = factor.astype(jnp.int32).astype(jnp.int16)


def project(chunks, x_ref, w_ref, out_ref, w_vmem, sems):
    seq_count = x_ref.shape[0]
    depth = w_vmem.shape[0]
    chunk = depth // chunks

    def copy(e):
        at = pl.ds(e * chunk, chunk)
        return pltpu.make_async_copy(w_ref.at[0, at], w_vmem.at[at], sems.at[e])

    def rows(lo, size):
        part = [x_ref[s - 1, :, lo : lo + size].astype(jnp.int32) for s in order]
        return jnp.concatenate(part, axis=0).astype(F32)

    order = [s or seq_count for s in range(seq_count)]

    for e in range(chunks):
        copy(e).start()
    factor = rows(depth, HD)
    factor = factor[:, 0:1] * F32(1 / DIGITS) * jnp.exp2(factor[:, 1:2])
    acc = jnp.zeros((seq_count * x_ref.shape[1], w_vmem.shape[1]), F32)
    for e in range(chunks):
        x = rows(e * chunk, chunk).astype(BF16)
        copy(e).wait()
        acc = acc + jnp.dot(
            x, w_vmem[e * chunk : (e + 1) * chunk], preferred_element_type=F32
        )
    upper = acc * factor
    act = (upper / (1.0 + jnp.exp(-upper))).reshape(-1, PEERS, upper.shape[1])
    tiles = upper.shape[1] // HD
    parts = [act[:, :, j * HD : (j + 1) * HD] for j in range(tiles)]
    parts += [jnp.zeros_like(parts[0])] * (PEERS - tiles)
    turned = jnp.swapaxes(jnp.stack(parts, axis=1), 1, 2).astype(BF16)
    slots = out_ref.shape[1] // PEERS
    for s in range(seq_count):
        for c in range(slots):
            at = pl.ds(c * PEERS, PEERS)
            out_ref[s * PEERS : (s + 1) * PEERS, at] = turned[s * slots + c]


def mix(back_ref, selector_ref, column_ref, out_ref):
    seq_count = back_ref.shape[0] // PEERS
    units = out_ref.shape[1] // seq_count
    tiles = units // HD
    rows = selector_ref.shape[0]
    selectors = selector_ref[...]
    for s in range(seq_count):
        back = back_ref[s * PEERS : (s + 1) * PEERS].astype(F32)
        back = jnp.swapaxes(back.reshape(rows // PEERS, PEERS, PEERS, HD), 1, 2)
        wide = [back[:, j].reshape(rows, HD) for j in range(tiles)]
        wide = jnp.concatenate(wide, axis=1).astype(BF16)
        picked = lax.dot_general(
            selectors, wide, (((0,), (0,)), ((), ())), preferred_element_type=F32
        )
        both = picked[:PEERS] * column_ref[0, :, 0:1] + picked[PEERS:] * column_ref[1, :, 0:1]
        out_ref[:, s * units : (s + 1) * units] = both.astype(BF16)


def shards(queries, keys, values, lengths, routes, gates, w_up):
    q_rows, width = queries.shape
    shard_len = keys.shape[0]
    seq_count = lax.axis_size("seq")
    expert_count = lax.axis_size("expert")
    capacity = 3
    tok_count = routes.shape[0]
    per_expert = expert_count * capacity
    reach = LONGEST + shard_len
    reach = reach - (shard_len - q_rows)

    heads = width // HD
    keys, values, queries, lengths, routes, gates = (
        pltpu.with_memory_space_constraint(x, pltpu.HBM)
        for x in (keys, values, queries, lengths.reshape(1, -1), routes.T, gates.T)
    )
    hbm = pl.BlockSpec(memory_space=pltpu.HBM)
    small = pltpu.CompilerParams(vmem_limit_bytes=8 << 20)
    left_rows = 2 * shard_len + heads * q_rows + ROUTE_ROWS
    own, left = pl.pallas_call(
        first,
        out_shape=(
            jax.ShapeDtypeStruct((2, shard_len, HD), BF16),
            jax.ShapeDtypeStruct((left_rows, HD), BF16),
        ),
        in_specs=[hbm] * 4,
        out_specs=(VMEM,) * 2,
        scratch_shapes=[
            pltpu.VMEM(routes.shape, jnp.int32),
            pltpu.SemaphoreType.DMA((5 + heads,)),
        ],
        compiler_params=small,
        name="first",
    )(keys, values, queries, routes)
    bounds = pl.pallas_call(
        functools.partial(second, shard_len, q_rows),
        out_shape=(
            jax.ShapeDtypeStruct((q_rows, HD), jnp.int32),
            jax.ShapeDtypeStruct((per_expert, 2 * tok_count), BF16),
            jax.ShapeDtypeStruct((2, tok_count, HD), F32),
        ),
        in_specs=[hbm] * 3,
        out_specs=(VMEM,) * 3,
        scratch_shapes=[
            pltpu.VMEM(lengths.shape, jnp.int32),
            pltpu.VMEM(routes.shape, jnp.int32),
            pltpu.VMEM(gates.shape, F32),
            pltpu.SemaphoreType.DMA((3,)),
        ],
        compiler_params=small,
        cost_estimate=pl.CostEstimate(flops=4_000_000, bytes_accessed=200_000, transcendentals=0),
        name="second",
    )(lengths, routes, gates)
    begin, selectors, columns = bounds

    def shifted(x, by):
        return lax.ppermute(x, "seq", [(i, (i + by) % seq_count) for i in range(seq_count)])

    near = shifted(own, 1)
    came = shifted(left, -1)
    beyond = pl.pallas_call(
        forward,
        out_shape=jax.ShapeDtypeStruct((2, reach - 3 * shard_len, HD), BF16),
        in_specs=[VMEM] * 2,
        out_specs=VMEM,
        compiler_params=small,
        name="forward",
    )(own, near)
    beyond = shifted(beyond, 2)
    message = pl.pallas_call(
        spread,
        out_shape=jax.ShapeDtypeStruct((expert_count, 2, tok_count), jnp.int32),
        in_specs=[VMEM],
        out_specs=VMEM,
        compiler_params=small,
        name="spread",
    )(came)
    row_routes = exchange(message, "expert")

    attended = pl.pallas_call(
        attend,
        out_shape=jax.ShapeDtypeStruct((q_rows, width), BF16),
        in_specs=[VMEM] * 5,
        out_specs=VMEM,
        compiler_params=pltpu.CompilerParams(vmem_limit_bytes=24 << 20),
        cost_estimate=pl.CostEstimate(
            flops=4 * heads * q_rows * reach * HD, bytes_accessed=0, transcendentals=0
        ),
        name="attend",
    )(begin, came, own, near, beyond)
    outgoing = pl.pallas_call(
        select,
        out_shape=jax.ShapeDtypeStruct((expert_count, per_expert, width), BF16),
        in_specs=[VMEM] * 2,
        out_specs=VMEM,
        compiler_params=small,
        name="select",
    )(attended, row_routes)
    landed = exchange(outgoing, "expert")
    packed = pl.pallas_call(
        pack,
        out_shape=jax.ShapeDtypeStruct((per_expert, expert_count * width + HD), jnp.int16),
        in_specs=[VMEM],
        out_specs=VMEM,
        compiler_params=pltpu.CompilerParams(vmem_limit_bytes=16 << 20),
        name="pack",
    )(landed)
    incoming = lax.all_gather(packed, "seq")
    act = pl.pallas_call(
        functools.partial(project, expert_count),
        out_shape=jax.ShapeDtypeStruct((seq_count * expert_count, per_expert, HD), BF16),
        in_specs=[VMEM, pl.BlockSpec(memory_space=pltpu.HBM)],
        out_specs=VMEM,
        scratch_shapes=[
            pltpu.VMEM(w_up.shape[1:], BF16),
            pltpu.SemaphoreType.DMA((expert_count,)),
        ],
        compiler_params=pltpu.CompilerParams(vmem_limit_bytes=32 << 20),
        name="project",
    )(incoming, pltpu.with_memory_space_constraint(w_up, pltpu.HBM))
    back = exchange(act, ("seq", "expert"))
    return pl.pallas_call(
        mix,
        out_shape=jax.ShapeDtypeStruct((tok_count, seq_count * w_up.shape[2]), BF16),
        in_specs=[VMEM] * 3,
        out_specs=VMEM,
        compiler_params=pltpu.CompilerParams(vmem_limit_bytes=16 << 20),
        name="mix",
    )(back, selectors, columns)


def solution(mesh):
    placed = (
        P(("dp", "seq"), "expert"),
        P(("dp", "seq"), "expert"),
        P(("dp", "seq"), "expert"),
        P("dp"),
        P(("dp", "seq", "expert"), None),
        P(("dp", "seq", "expert"), None),
        P("expert", None, "seq"),
    )

    return jax.shard_map(
        shards,
        mesh=mesh,
        in_specs=placed,
        out_specs=P(("dp", "seq", "expert"), None),
        check_vma=False,
    )
```
